32 devices in a mesh: dom: 8 (over z, y), edge: 4 (over x, core).
Axes of the slice: x: 2, y: 2, z: 4, core: 2. Of those that a mesh axis runs over, the one named last changes fastest.
Arguments:
- fine_nodes: bfloat16 [65536, 128], P('dom'), may hold values from -6 to 6
- fine_edges: bfloat16 [131072, 128], P(('dom', 'edge')), may hold values from -6 to 6
- fine_senders: int32 [131072], P(('dom', 'edge')), may hold values from 0 to 8703, as said below
- fine_receivers: int32 [131072], P(('dom', 'edge')), may hold values from 0 to 8191
- fine_halo: int32 [8, 8, 64], P('dom'), may hold values from 0 to 8191
- coarse_edges: bfloat16 [32768, 128], P(('dom', 'edge')), may hold values from -6 to 6
- coarse_senders: int32 [32768], P(('dom', 'edge')), may hold values from 0 to 2303, as said below
- coarse_receivers: int32 [32768], P(('dom', 'edge')), may hold values from 0 to 2047
- coarse_halo: int32 [8, 8, 32], P('dom'), may hold values from 0 to 2047
- pool_send: int32 [8, 8, 1536], P('dom'), may hold values from 0 to 8191, as said below
- pool_dest: int32 [8, 8, 1536], P('dom'), may hold values from 0 to 2048, as said below
- unpool_slot: int32 [65536], P('dom'), may hold values from 0 to 12287, as said below
- edge_in_weight: bfloat16 [2, 384, 128], replicated, may hold values from -0.3125 to 0.3125
- edge_out_weight: bfloat16 [2, 128, 128], replicated, may hold values from -0.5 to 0.5
- node_in_weight: bfloat16 [2, 256, 128], replicated, may hold values from -0.375 to 0.375
- node_out_weight: bfloat16 [2, 128, 128], replicated, may hold values from -0.5 to 0.5
- edge_gain: float32 [2, 128], replicated, may hold values from 0.5 to 1.5
- node_gain: float32 [2, 128], replicated, may hold values from 0.5 to 1.5
Outputs:
- fine_out: bfloat16 [65536, 128], P('dom')
- coarse_out: bfloat16 [16384, 128], P('dom')
The draws below stay inside these ranges and needn't reach their ends.
Inputs may be any that keep to these rules, and one draw needn't show every extreme that they name: `fine_senders`: an entry below 8192 is a row of the edge's own partition; an entry 8192 + d * 64 + s names slot s of fine_halo[d, p] for the edge's partition p. `coarse_senders`: an entry below 2048 is a row of the edge's own coarse partition; an entry 2048 + d * 32 + s names slot s of coarse_halo[d, p]. pool_send[d, p, s] is a row of partition d. For each pair (d, p) the slots that carry data come first and number at most 1536; in every draw some p receives 1536 from every d. Every row of partition d is carried exactly once over all p and s; empty slots hold 0. pool_dest[p, d, s] is 2048 exactly where slot s of pool_send[d, p] is empty, else a row of coarse partition p. `unpool_slot`: row r of partition d holds p * 1536 + s for the one carrying slot with pool_send[d, p, s] = r.
All inputs are finite; a program needn't handle non-finite values.
Results may differ from the reference program's by a relative error of at most 0.0068.
Values may be sent and summed in bfloat16 or wider, within the bound.
No kernel may reach another device: no remote copies, remote signals or barrier semaphores. Data moves between devices by JAX's collectives and lax.ppermute only.
A program may use at most 64 MiB of HBM per device.

```python
import jax
import jax.numpy as jnp
from jax import lax

H = 128
FINE_DEV = 8192
EDGE_DEV = 4096
COARSE = 2048
CEDGE_DEV = 1024
HALO = 64
CHALO = 32
GHOSTS = 512
CGHOSTS = 256
PS = 1536
NF = 65536
NE = 131072
NCE = 32768
N_DOM = 8
N_EDGE = 4


def sender_mix(key, rows, ghosts, total):
    first, second, third = jax.random.split(key, 3)
    near = jax.random.randint(first, (total,), 0, rows, dtype=jnp.int32)
    far = rows + jax.random.randint(second, (total,), 0, ghosts, dtype=jnp.int32)
    pick = jax.random.randint(third, (total,), 0, 4, dtype=jnp.int32)
    return jnp.where(pick == 0, far, near).astype(jnp.int32)


def draw_fine_senders(key, part):
    return sender_mix(jax.random.fold_in(key, 11), FINE_DEV, GHOSTS, EDGE_DEV * N_DOM * N_EDGE)


def draw_coarse_senders(key, part):
    return sender_mix(jax.random.fold_in(key, 12), COARSE, CGHOSTS, CEDGE_DEV * N_DOM * N_EDGE)


def pool_layout(key):
    base_key = jax.random.fold_in(key, 7)
    first, second, third, fourth = jax.random.split(base_key, 4)
    pairs = N_DOM // 2
    base = FINE_DEV // N_DOM
    small = base // 2
    chosen = jax.random.randint(first, (), 0, pairs, dtype=jnp.int32)
    flips = jax.random.randint(second, (N_DOM, pairs), 0, 2, dtype=jnp.int32)
    flips = jnp.where(jnp.arange(pairs, dtype=jnp.int32)[None, :] == chosen, 1, flips)
    even_count = jnp.where(flips == 1, PS, small)
    odd_count = jnp.where(flips == 1, small, PS)
    counts = jnp.stack([even_count, odd_count], axis=-1).reshape(N_DOM, N_DOM).astype(jnp.int32)
    starts = (jnp.cumsum(counts, axis=1) - counts).astype(jnp.int32)
    orders = jax.vmap(lambda k: jax.random.permutation(k, jnp.arange(FINE_DEV, dtype=jnp.int32)))(jax.random.split(third, N_DOM))
    slots = jnp.arange(PS, dtype=jnp.int32)
    valid = slots[None, None, :] < counts[:, :, None]
    spots = jnp.minimum(starts[:, :, None] + slots[None, None, :], FINE_DEV - 1)
    picked = jax.vmap(lambda order, spot: order[spot])(orders, spots)
    send = jnp.where(valid, picked, 0).astype(jnp.int32)
    ranks = jnp.arange(FINE_DEV, dtype=jnp.int32)

    def slot_of(start, order):
        owner = (jnp.sum((start[None, :] <= ranks[:, None]).astype(jnp.int32), axis=1) - 1).astype(jnp.int32)
        offset = ranks - start[owner]
        value = (owner * PS + offset).astype(jnp.int32)
        return jnp.zeros((FINE_DEV,), jnp.int32).at[order].set(value)
    unpool = jax.vmap(slot_of)(starts, orders).reshape(-1).astype(jnp.int32)
    places = jax.random.randint(fourth, (N_DOM, N_DOM, PS), 0, COARSE, dtype=jnp.int32)
    dest = jnp.where(jnp.transpose(valid, (1, 0, 2)), places, COARSE).astype(jnp.int32)
    return (send, dest, unpool)


def draw_pool_send(key, part):
    return pool_layout(key)[0]


def draw_pool_dest(key, part):
    return pool_layout(key)[1]


def draw_unpool_slot(key, part):
    return pool_layout(key)[2]


def touch_ends(drawn, rng, low, top_value):
    dims = drawn.shape
    spot = [jax.random.randint(jax.random.fold_in(rng, axis), (), 0, dims[axis]) for axis in range(len(dims))]
    drawn = drawn.at[tuple(spot)].set(low)
    longest = dims.index(max(dims))
    spot[longest] = (spot[longest] + 1) % dims[longest]
    return drawn.at[tuple(spot)].set(top_value)


def steps_of(stream_key, shape, pieces, least, high):
    level = 1.0
    for axis_at, blocks in pieces:
        draws = jax.random.uniform(jax.random.fold_in(jax.random.fold_in(stream_key, 6), axis_at), (blocks,), jnp.float32, least / len(pieces), high / len(pieces))
        level = level * jnp.repeat(jnp.exp(draws), shape[axis_at] // blocks).reshape((-1,) + (1,) * (len(shape) - 1 - axis_at))
    return level


def noise(rng, shape, scale, limit, shards=(), kind=jnp.bfloat16):
    entries = scale * jax.random.normal(rng, shape, jnp.float32)
    if shards:
        entries = entries * steps_of(rng, shape, shards, -0.22, 0.18)
    return jnp.clip(entries, -limit, limit).astype(kind)


def setup_inputs(seed: int = 0) -> dict:
    key_list = jax.random.split(jax.random.key(seed), 19)
    fine_nodes = noise(key_list[0], (NF, H), 1.0, 6.0, ((0, 8),))
    fine_edges = noise(key_list[1], (NE, H), 1.0, 6.0, ((0, 32),))
    fine_senders = draw_fine_senders(jax.random.fold_in(key_list[18], 71), 0)
    fine_receivers = touch_ends(jax.random.randint(key_list[3], (NE,), 0, FINE_DEV), jax.random.fold_in(key_list[3], 1), 0, FINE_DEV - 1).astype(jnp.int32)
    fine_halo = touch_ends(jax.random.randint(key_list[4], (N_DOM, N_DOM, HALO), 0, FINE_DEV), jax.random.fold_in(key_list[4], 1), 0, FINE_DEV - 1).astype(jnp.int32)
    coarse_edges = noise(key_list[5], (NCE, H), 1.0, 6.0, ((0, 32),))
    coarse_senders = draw_coarse_senders(jax.random.fold_in(key_list[18], 71), 0)
    coarse_receivers = touch_ends(jax.random.randint(key_list[7], (NCE,), 0, COARSE), jax.random.fold_in(key_list[7], 1), 0, COARSE - 1).astype(jnp.int32)
    coarse_halo = touch_ends(jax.random.randint(key_list[8], (N_DOM, N_DOM, CHALO), 0, COARSE), jax.random.fold_in(key_list[8], 1), 0, COARSE - 1).astype(jnp.int32)
    pool_send = draw_pool_send(jax.random.fold_in(key_list[18], 71), 0)
    pool_dest = draw_pool_dest(jax.random.fold_in(key_list[18], 71), 0)
    unpool_slot = draw_unpool_slot(jax.random.fold_in(key_list[18], 71), 0)
    edge_in_weight = noise(key_list[12], (2, 3 * H, H), (3 * H) ** -0.5, 0.3125)
    edge_out_weight = noise(key_list[13], (2, H, H), H ** -0.5, 0.5)
    node_in_weight = noise(key_list[14], (2, 2 * H, H), (2 * H) ** -0.5, 0.375)
    node_out_weight = noise(key_list[15], (2, H, H), H ** -0.5, 0.5)
    edge_gain = jnp.clip(1.0 + 0.1 * jax.random.normal(key_list[16], (2, H), jnp.float32), 0.5, 1.5)
    node_gain = jnp.clip(1.0 + 0.1 * jax.random.normal(key_list[17], (2, H), jnp.float32), 0.5, 1.5)
    return {"fine_nodes": fine_nodes, "fine_edges": fine_edges, "fine_senders": fine_senders, "fine_receivers": fine_receivers, "fine_halo": fine_halo, "coarse_edges": coarse_edges, "coarse_senders": coarse_senders, "coarse_receivers": coarse_receivers, "coarse_halo": coarse_halo, "pool_send": pool_send, "pool_dest": pool_dest, "unpool_slot": unpool_slot, "edge_in_weight": edge_in_weight, "edge_out_weight": edge_out_weight, "node_in_weight": node_in_weight, "node_out_weight": node_out_weight, "edge_gain": edge_gain, "node_gain": node_gain}


def layer_norm(values, gain):
    center = values - lax.optimization_barrier(jnp.mean(values, axis=-1, keepdims=True))
    spread = lax.optimization_barrier(jnp.mean(center * center, axis=-1, keepdims=True))
    return center * lax.rsqrt(spread + 1e-05) * gain

def node_update(rows, summed, w_first, w_second, gain):
    inputs = jnp.concatenate([rows, summed.astype(jnp.bfloat16)], axis=1)
    hidden = jax.nn.silu(jnp.dot(inputs, w_first, preferred_element_type=jnp.float32)).astype(jnp.bfloat16)
    result = layer_norm(jnp.dot(hidden, w_second, preferred_element_type=jnp.float32), gain)
    return (rows.astype(jnp.float32) + result).astype(jnp.bfloat16)

def graph_layer(nodes, edges, senders, receivers, border, level, weights):
    edge_in_weight, edge_out_weight, node_in_weight, node_out_weight, edge_gain, node_gain = weights
    width = nodes.shape[-1]
    parts = nodes.reshape(N_DOM, -1, width)
    row_count = parts.shape[1]
    sent = jax.vmap(lambda rows, index: rows[index])(parts, border)
    ghosts = jnp.transpose(sent, (1, 0, 2, 3)).reshape(N_DOM, -1, width)
    edge_parts = edges.reshape(N_DOM, -1, width)
    send_parts = senders.reshape(N_DOM, -1)
    recv_parts = receivers.reshape(N_DOM, -1)

    def one_part(items):
        rows, ghost, edge_rows, sender, receiver = items
        table = jnp.concatenate([rows, ghost], axis=0)
        inputs = jnp.concatenate([table[sender], rows[receiver], edge_rows], axis=1)
        hidden = jax.nn.silu(jnp.dot(inputs, edge_in_weight[level], preferred_element_type=jnp.float32)).astype(jnp.bfloat16)
        message = layer_norm(jnp.dot(hidden, edge_out_weight[level], preferred_element_type=jnp.float32), edge_gain[level])
        summed = jax.ops.segment_sum(message, receiver, num_segments=row_count)
        return node_update(rows, summed, node_in_weight[level], node_out_weight[level], node_gain[level])
    result = lax.map(one_part, (parts, ghosts, edge_parts, send_parts, recv_parts))
    return result.reshape(-1, width)

def reference(fine_nodes, fine_edges, fine_senders, fine_receivers, fine_halo, coarse_edges, coarse_senders, coarse_receivers, coarse_halo, pool_send, pool_dest, unpool_slot, edge_in_weight, edge_out_weight, node_in_weight, node_out_weight, edge_gain, node_gain):
    weights = (edge_in_weight, edge_out_weight, node_in_weight, node_out_weight, edge_gain, node_gain)
    width = fine_nodes.shape[-1]
    fine_mid = graph_layer(fine_nodes, fine_edges, fine_senders, fine_receivers, fine_halo, 0, weights)
    mid_parts = fine_mid.reshape(N_DOM, -1, width)

    def pool_one(target):
        rows = jax.vmap(lambda part, index: part[index])(mid_parts, pool_send[:, target, :])
        places = pool_dest[target].reshape(-1)
        sums = jax.ops.segment_sum(rows.reshape(-1, width).astype(jnp.float32), places, num_segments=COARSE + 1)[:COARSE]
        counts = jax.ops.segment_sum(jnp.ones_like(places), places, num_segments=COARSE + 1)[:COARSE]
        return (sums / jnp.maximum(counts, 1).astype(jnp.float32)[:, None]).astype(jnp.bfloat16)
    coarse_in = lax.map(pool_one, jnp.arange(N_DOM, dtype=jnp.int32)).reshape(-1, width)
    coarse_out = graph_layer(coarse_in, coarse_edges, coarse_senders, coarse_receivers, coarse_halo, 1, weights)
    source = (jnp.arange(NF, dtype=jnp.int32) // FINE_DEV).astype(jnp.int32)
    target = (unpool_slot // PS).astype(jnp.int32)
    within = (unpool_slot % PS).astype(jnp.int32)
    place = pool_dest[target, source, within]
    parents = coarse_out[(target * COARSE + place).astype(jnp.int32)]
    fine_out = (fine_mid.astype(jnp.float32) + parents.astype(jnp.float32)).astype(jnp.bfloat16)
    return (fine_out, coarse_out)
```

```python
import jax
import jax.numpy as jnp
from jax import lax
from jax.experimental import pallas as pl
from jax.experimental.pallas import tpu as pltpu
from jax.sharding import PartitionSpec as P

BF = jnp.bfloat16
F32 = jnp.float32
VMEM = pl.BlockSpec(memory_space=pltpu.VMEM)
SMEM = pl.BlockSpec(memory_space=pltpu.SMEM)
COARSE = 2048
UNROLL = 16
ACCS = 4


def call(kernel, out_shape, in_specs, scratch=(), name=None):
    outs = jax.tree.map(lambda _: VMEM, out_shape)
    return pl.pallas_call(
        kernel,
        out_shape=out_shape,
        in_specs=in_specs,
        out_specs=outs,
        scratch_shapes=list(scratch),
        name=name,
        compiler_params=pltpu.CompilerParams(vmem_limit_bytes=60 * 1024 * 1024),
    )


def shaped(rows, dtype, width=128):
    return jax.ShapeDtypeStruct((rows, width), dtype)


def dot(a, b):
    return jnp.dot(a, b, preferred_element_type=F32)


def silu(v):
    return v / (1.0 + jnp.exp(-v))


def norm(values, gain):
    center = values - jnp.mean(values, axis=-1, keepdims=True)
    spread = jnp.mean(center * center, axis=-1, keepdims=True)
    return center * lax.rsqrt(spread + 1e-05) * gain


def blocks(total, size, body):
    size = min(size, total)

    def step(i, carry):
        body(pl.multiple_of(i * size, size))
        return carry

    lax.fori_loop(0, total // size, step, 0)


def edge_gather(nodes, edges, near, receivers, w_in):
    rows, width = nodes.shape
    count = edges.shape[0]

    def kernel(near_ref, recv_ref, nodes_ref, edges_ref, w_ref, out_ref, send_tab, recv_tab):
        w_s = w_ref[0:width, :]
        w_r = w_ref[width : 2 * width, :]
        w_e = w_ref[2 * width : 3 * width, :]

        def project(at):
            block = nodes_ref[pl.ds(at, min(512, rows)), :]
            send_tab[pl.ds(at, min(512, rows)), :] = dot(block, w_s)
            recv_tab[pl.ds(at, min(512, rows)), :] = dot(block, w_r)

        blocks(rows, 512, project)
        send_tab[pl.ds(rows, 8), :] = jnp.zeros((8, width), F32)

        def gather(i, carry):
            base = i * UNROLL
            for j in range(UNROLL):
                s = near_ref[base + j]
                r = recv_ref[base + j]
                out_ref[pl.ds(base + j, 1), :] = send_tab[pl.ds(s, 1), :] + recv_tab[pl.ds(r, 1), :]
            return carry

        lax.fori_loop(0, count // UNROLL, gather, 0)

        def add_edges(at):
            n = min(512, count)
            out_ref[pl.ds(at, n), :] = out_ref[pl.ds(at, n), :] + dot(edges_ref[pl.ds(at, n), :], w_e)

        blocks(count, 512, add_edges)

    return call(
        kernel,
        shaped(count, F32),
        [SMEM, SMEM, VMEM, VMEM, VMEM],
        [pltpu.VMEM((rows + 8, width), F32), pltpu.VMEM((rows, width), F32)],
        "edge_gather",
    )(near, receivers, nodes, edges, w_in)


def edge_message(pre, ghosts, far, receivers, table, w_in, w_out, gain, slots, mapped):
    count, width = pre.shape
    ghost_rows = ghosts.shape[0]
    half = slots // 2
    n = min(256, count)

    def kernel(recv_ref, table_ref, far_ref, pre_ref, ghost_ref, w_ref, wo_ref, gain_ref, keep_ref, send_ref, msg, *accs):
        def clear(at):
            for acc in accs:
                acc[pl.ds(at, 512), :] = jnp.zeros((512, width), F32)

        blocks(slots, 512, clear)
        w_s = w_ref[0:width, :]
        w_o = wo_ref[...]

        def message(at):
            pick = (far_ref[pl.ds(at, n), :] == lax.broadcasted_iota(jnp.int32, (n, ghost_rows), 1)).astype(BF)
            picked = dot(pick, ghost_ref[...]).astype(BF)
            hidden = silu(pre_ref[pl.ds(at, n), :] + dot(picked, w_s)).astype(BF)
            msg[pl.ds(at, n), :] = norm(dot(hidden, w_o), gain_ref[...])

        blocks(count, n, message)

        def scatter(i, carry):
            base = i * UNROLL
            for j in range(UNROLL):
                acc = accs[j % ACCS]
                r = recv_ref[base + j]
                if mapped:
                    r = table_ref[r]
                acc[pl.ds(r, 1), :] = acc[pl.ds(r, 1), :] + msg[pl.ds(base + j, 1), :]
            return carry

        lax.fori_loop(0, count // UNROLL, scatter, 0)

        def finish(at):
            m = min(512, half)
            low = accs[0][pl.ds(at, m), :]
            high = accs[0][pl.ds(at + half, m), :]
            for acc in accs[1:]:
                low = low + acc[pl.ds(at, m), :]
                high = high + acc[pl.ds(at + half, m), :]
            keep_ref[pl.ds(at, m), :] = low
            send_ref[pl.ds(at, m), :] = high.astype(BF)

        blocks(half, 512, finish)

    return call(
        kernel,
        (shaped(half, F32), shaped(half, BF)),
        [SMEM, SMEM] + [VMEM] * 6,
        [pltpu.VMEM((count, width), F32)] + [pltpu.VMEM((slots, width), F32)] * ACCS,
        "edge_message",
    )(receivers, table, far.reshape(count, 1), pre, ghosts, w_in, w_out, gain)


def node_update(rows, kept, first, second, w_in, w_out, gain):
    count, width = rows.shape
    n = min(256, count)

    def kernel(rows_ref, kept_ref, first_ref, second_ref, w_ref, wo_ref, gain_ref, out_ref):
        def step(at):
            own = rows_ref[pl.ds(at, n), :]
            total = (
                kept_ref[pl.ds(at, n), :]
                + first_ref[pl.ds(at, n), :].astype(F32)
                + second_ref[pl.ds(at, n), :].astype(F32)
            ).astype(BF)
            hidden = silu(dot(own, w_ref[0:width, :]) + dot(total, w_ref[width : 2 * width, :])).astype(BF)
            result = norm(dot(hidden, wo_ref[...]), gain_ref[...])
            out_ref[pl.ds(at, n), :] = (own.astype(F32) + result).astype(BF)

        blocks(count, n, step)

    return call(kernel, shaped(count, BF), [VMEM] * 7, (), "node_update")(
        rows, kept, first, second, w_in, w_out, gain
    )


def take_rows(table, index):
    rows, width = table.shape
    count = index.shape[0]

    def kernel(index_ref, table_ref, out_ref, wide, picked):
        def widen(at):
            wide[pl.ds(at, 256), :] = table_ref[pl.ds(at, 256), :].astype(F32)

        blocks(rows, 256, widen)

        def gather(i, carry):
            base = i * UNROLL
            for j in range(UNROLL):
                picked[pl.ds(base + j, 1), :] = wide[pl.ds(index_ref[base + j], 1), :]
            return carry

        lax.fori_loop(0, count // UNROLL, gather, 0)

        def narrow(at):
            out_ref[pl.ds(at, 256), :] = picked[pl.ds(at, 256), :].astype(BF)

        blocks(count, 256, narrow)

    return call(
        kernel,
        shaped(count, BF),
        [SMEM, VMEM],
        [pltpu.VMEM((rows, width), F32), pltpu.VMEM((count, width), F32)],
        "take_rows",
    )(index, table)


def pool_sum(arrived, places):
    count, width = arrived.shape
    n = 256

    def kernel(arrived_ref, places_ref, out_ref):
        rows = arrived_ref[...]

        def step(at):
            pick = (places_ref[...] == at + lax.broadcasted_iota(jnp.int32, (n, count), 0)).astype(BF)
            out_ref[pl.ds(at, n), :] = dot(pick, rows)

        blocks(COARSE, n, step)

    return call(kernel, shaped(COARSE, F32), [VMEM, VMEM], (), "pool_sum")(arrived, places.reshape(1, count))


def child_count(places):
    count = places.shape[0]
    high = (places // 128)[None, :] == jnp.arange(COARSE // 128, dtype=jnp.int32)[:, None]
    low = (places % 128)[:, None] == jnp.arange(128, dtype=jnp.int32)[None, :]
    return dot(high.astype(BF), low.astype(BF)).reshape(COARSE)


def swap(x, bit):
    size = lax.axis_size("edge")
    return lax.ppermute(x, "edge", [(i, i ^ bit) for i in range(size)])


def layer_sums(nodes, edges, senders, receivers, border, level, w, slots, table):
    rows, width = nodes.shape
    outgoing = nodes[border[0].reshape(-1)].reshape(border.shape[1], border.shape[2], width)
    arrived = lax.all_to_all(outgoing, "dom", split_axis=0, concat_axis=0, tiled=True)
    pre = edge_gather(nodes, edges, jnp.minimum(senders, rows), receivers, w[0][level])
    ghosts = arrived.reshape(-1, width)
    mapped = table is not None
    if mapped:
        index = receivers
    else:
        me = lax.axis_index("edge")
        quarter = rows // 4
        index = order_of((receivers // quarter) ^ me) * quarter + receivers % quarter
        table = index
    keep, send = edge_message(
        pre, ghosts, senders - rows, index, table, w[0][level], w[1][level], w[4][level][None], slots, mapped
    )
    first = swap(send, 1)
    half = slots // 4
    second = swap((keep[half:] + first[half:].astype(F32)).astype(BF), 2)
    return keep[:half], first[:half], second


def order_of(rel):
    return (rel & 1) * 2 + (rel >> 1)


def shards(
    fine_nodes,
    fine_edges,
    fine_senders,
    fine_receivers,
    fine_halo,
    coarse_edges,
    coarse_senders,
    coarse_receivers,
    coarse_halo,
    pool_send,
    pool_dest,
    unpool_slot,
    edge_in_weight,
    edge_out_weight,
    node_in_weight,
    node_out_weight,
    edge_gain,
    node_gain,
):
    w = (edge_in_weight, edge_out_weight, node_in_weight, node_out_weight, edge_gain, node_gain)
    width = fine_nodes.shape[-1]
    n_dom = pool_send.shape[1]
    span = pool_send.shape[2]
    part = span // 4
    slots = n_dom * span
    quarter = n_dom * part
    me = lax.axis_index("edge")
    target = unpool_slot // span
    within = unpool_slot % span
    slot_place = order_of((within // part) ^ me) * quarter + target * part + within % part
    my_send = lax.dynamic_slice_in_dim(pool_send[0], me * part, part, 1).reshape(-1)
    my_dest = lax.dynamic_slice_in_dim(pool_dest[0], me * part, part, 1).reshape(-1)
    counts = child_count(pool_dest[0].reshape(-1))
    scale = jnp.maximum(counts, 1.0)[:, None]

    kept, first, second = layer_sums(
        fine_nodes, fine_edges, fine_senders, fine_receivers, fine_halo, 0, w, slots, slot_place
    )
    own = take_rows(fine_nodes, my_send)
    mid = node_update(own, kept, first, second, w[2][0], w[3][0], w[5][0][None])

    arrived = lax.all_to_all(mid.reshape(n_dom, part, width), "dom", split_axis=0, concat_axis=0, tiled=True)
    sums = pool_sum(arrived.reshape(-1, width), my_dest)
    bit = me & 1
    half = COARSE // 2
    mine = lax.dynamic_slice_in_dim(sums, bit * half, half, 0)
    theirs = lax.dynamic_slice_in_dim(sums, (1 - bit) * half, half, 0)
    mine = mine + swap(theirs, 1)
    mine = mine + swap(mine.astype(BF), 2).astype(F32)
    mine = (mine / lax.dynamic_slice_in_dim(scale, bit * half, half, 0)).astype(BF)
    theirs = swap(mine, 1)
    coarse_in = jnp.concatenate([jnp.where(bit == 0, mine, theirs), jnp.where(bit == 0, theirs, mine)], axis=0)

    kept, first, second = layer_sums(
        coarse_in, coarse_edges, coarse_senders, coarse_receivers, coarse_halo, 1, w, COARSE, None
    )
    fourth = COARSE // 4
    own = lax.dynamic_slice_in_dim(coarse_in, me * fourth, fourth, 0)
    top = node_update(own, kept, first, second, w[2][1], w[3][1], w[5][1][None])
    coarse_out = lax.all_gather(top, "edge", axis=0, tiled=True)

    parents = take_rows(coarse_out, jnp.minimum(my_dest, COARSE - 1))
    back = lax.all_to_all(parents.reshape(n_dom, part, width), "dom", split_axis=0, concat_axis=0, tiled=True)
    final = (mid.astype(F32) + back.reshape(-1, width).astype(F32)).astype(BF)
    pair = jnp.concatenate([final, swap(final, 2)], axis=0)
    table = jnp.concatenate([pair, swap(pair, 1)], axis=0)
    fine_out = take_rows(table, slot_place)
    return (fine_out, coarse_out)


def solution(mesh):
    placed = (
        P("dom", None),
        P(("dom", "edge"), None),
        P(("dom", "edge")),
        P(("dom", "edge")),
        P("dom", None, None),
        P(("dom", "edge"), None),
        P(("dom", "edge")),
        P(("dom", "edge")),
        P("dom", None, None),
        P("dom", None, None),
        P("dom", None, None),
        P("dom"),
        P(),
        P(),
        P(),
        P(),
        P(),
        P(),
    )
    return jax.shard_map(
        shards,
        mesh=mesh,
        in_specs=placed,
        out_specs=(P("dom", None), P("dom", None)),
        check_vma=False,
    )
```

```python
import jax
import jax.numpy as jnp
from jax import lax
from jax.experimental import pallas as pl
from jax.experimental.pallas import tpu as pltpu
from jax.sharding import PartitionSpec as P

BF = jnp.bfloat16
F32 = jnp.float32
VMEM = pl.BlockSpec(memory_space=pltpu.VMEM)
SMEM = pl.BlockSpec(memory_space=pltpu.SMEM)
HBM = pl.BlockSpec(memory_space=pltpu.HBM)
INDEX = "index"
WEIGHT = "weight"
COARSE = 2048
UNROLL = 32
ACCS = 4


def nbytes(x):
    width = -(-x.shape[-1] // 128) * 128
    return x.size // x.shape[-1] * width * x.dtype.itemsize


class Late:
    def __init__(self, ref, copy):
        self.ref = ref
        self.wait = copy.wait


def call(kernel, out_shape, in_specs, scratch=(), name=None):
    def run(*args):
        late = [k for k, spec in enumerate(in_specs) if spec in (INDEX, WEIGHT)]
        homes = [
            (pltpu.SMEM if in_specs[k] is INDEX else pltpu.VMEM)(args[k].shape, args[k].dtype) for k in late
        ]
        used = sum(nbytes(x) for x, spec in zip(args, in_specs) if spec is VMEM or spec is WEIGHT)
        used += sum(nbytes(x) for x in jax.tree.leaves(out_shape) if len(x.shape) > 1)
        used += sum(nbytes(x) for x in scratch)
        n_out = len(jax.tree.leaves(out_shape))

        def body(*refs):
            ins, outs = list(refs[: len(args)]), refs[len(args) : len(args) + n_out]
            mine = refs[len(args) + n_out : len(args) + n_out + len(scratch)]
            rest = refs[len(args) + n_out + len(scratch) :]
            for at, k in enumerate(late):
                copy = pltpu.make_async_copy(ins[k], rest[at], rest[len(late) + at])
                copy.start()
                ins[k] = Late(rest[at], copy)
            kernel(*ins, *outs, *mine)

        return pl.pallas_call(
            body,
            out_shape=out_shape,
            in_specs=[HBM if spec in (INDEX, WEIGHT) else spec for spec in in_specs],
            out_specs=jax.tree.map(lambda x: VMEM if len(x.shape) > 1 else SMEM, out_shape),
            scratch_shapes=[pltpu.VMEM(x.shape, x.dtype) for x in scratch]
            + homes
            + [pltpu.SemaphoreType.DMA(())] * len(late),
            name=name,
            compiler_params=pltpu.CompilerParams(vmem_limit_bytes=used + 2 * 1024 * 1024),
        )(*args)

    return run


def shaped(rows, dtype, width=128):
    return jax.ShapeDtypeStruct((rows, width), dtype)


def dot(a, b):
    return jnp.dot(a, b, preferred_element_type=F32)


def silu(v):
    return v / (1.0 + jnp.exp(-v))


def norm(values, gain):
    center = values - jnp.mean(values, axis=-1, keepdims=True)
    spread = jnp.mean(center * center, axis=-1, keepdims=True)
    return center * lax.rsqrt(spread + 1e-05) * gain


def blocks(total, size, body):
    size = min(size, total)

    def step(i, carry):
        body(pl.multiple_of(i * size, size))
        return carry

    lax.fori_loop(0, total // size, step, 0)


def edge_gather(nodes, senders, receivers, w_in, level, ghost_rows):
    rows, width = nodes.shape
    count = senders.shape[0]

    def kernel(send_idx, recv_idx, nodes_ref, w_late, out_ref, send_tab, recv_tab):
        send_tab[pl.ds(rows, ghost_rows), :] = jnp.zeros((ghost_rows, width), F32)
        w_late.wait()
        w_s = w_late.ref[level, 0:width, :]
        w_r = w_late.ref[level, width : 2 * width, :]

        def project(at):
            block = nodes_ref[pl.ds(at, 512), :]
            send_tab[pl.ds(at, 512), :] = dot(block, w_s)
            recv_tab[pl.ds(at, 512), :] = dot(block, w_r)

        blocks(rows, 512, project)
        send_idx.wait()
        recv_idx.wait()

        def gather(i, carry):
            base = i * UNROLL
            for j in range(UNROLL):
                s = send_idx.ref[base + j]
                r = recv_idx.ref[base + j]
                out_ref[pl.ds(base + j, 1), :] = send_tab[pl.ds(s, 1), :] + recv_tab[pl.ds(r, 1), :]
            return carry

        lax.fori_loop(0, count // UNROLL, gather, 0)

    return call(
        kernel,
        shaped(count, F32),
        [INDEX, INDEX, VMEM, WEIGHT],
        [shaped(rows + ghost_rows, F32), shaped(rows, F32)],
        "edge_gather",
    )(senders, receivers, nodes, w_in)


def edge_message(pre, edges, ghosts, senders, receivers, table, w_in, w_out, gain, level, rows, slots):
    count, width = pre.shape
    ghost_rows = ghosts.shape[0]
    fourth = slots // 4
    n = 256
    total = count // n
    mapped = table is not None

    def kernel(recv_idx, *refs):
        if mapped:
            table_idx, refs = refs[0], refs[1:]
        (send_late, pre_ref, edge_ref, ghost_ref, w_late, wo_late, gain_late,
         k0_ref, k2_ref, s1_ref, s3_ref, even, odd) = refs[:13]
        accs = refs[13:]

        def clear(at):
            for acc in accs:
                acc[pl.ds(at, 512), :] = jnp.zeros((512, width), F32)

        blocks(slots, 512, clear)
        send_late.wait()
        w_late.wait()
        wo_late.wait()
        gain_late.wait()
        w_s = w_late.ref[level, 0:width, :]
        w_e = w_late.ref[level, 2 * width : 3 * width, :]
        w_o = wo_late.ref[level]
        scale = gain_late.ref[level : level + 1, :]

        def message(b, msg):
            at = pl.multiple_of(b * n, n)
            columns = []
            for k in range(n // 128):
                far = (send_late.ref[pl.ds(b * (n // 128) + k, 1), :] - rows).astype(F32)
                columns.append(jnp.broadcast_to(far, (8, 128)).T[:, 0:1])
            column = jnp.concatenate(columns, axis=0)
            lane = lax.broadcasted_iota(jnp.int32, (n, ghost_rows), 1).astype(F32)
            pick = (column == lane).astype(BF)
            picked = dot(pick, ghost_ref[...]).astype(BF)
            first = pre_ref[pl.ds(at, n), :] + (dot(picked, w_s) + dot(edge_ref[pl.ds(at, n), :], w_e))
            msg[...] = norm(dot(silu(first).astype(BF), w_o), scale)

        def scatter(b, msg):
            base = b * n
            for j in range(n):
                acc = accs[j % ACCS]
                r = recv_idx.ref[base + j]
                if mapped:
                    r = table_idx.ref[r]
                acc[pl.ds(r, 1), :] = acc[pl.ds(r, 1), :] + msg[pl.ds(j, 1), :]

        message(0, even)
        recv_idx.wait()
        if mapped:
            table_idx.wait()

        def step(i, carry):
            b = 2 * i
            message(b + 1, odd)
            scatter(b, even)
            message(jnp.minimum(b + 2, total - 1), even)
            scatter(b + 1, odd)
            return carry

        lax.fori_loop(0, total // 2, step, 0)
        for place, out_ref in ((3, s3_ref), (1, k2_ref), (2, s1_ref), (0, k0_ref)):
            m = 256 if fourth % 256 == 0 else fourth

            def body(at, out_ref=out_ref, start=place * fourth, m=m):
                value = accs[0][pl.ds(at + start, m), :]
                for acc in accs[1:]:
                    value = value + acc[pl.ds(at + start, m), :]
                out_ref[pl.ds(at, m), :] = value.astype(out_ref.dtype)

            blocks(fourth, m, body)

    maps = [INDEX, INDEX] if mapped else [INDEX]
    index = (receivers, table) if mapped else (receivers,)
    return call(
        kernel,
        (shaped(fourth, F32), shaped(fourth, F32), shaped(fourth, BF), shaped(fourth, BF)),
        maps + [WEIGHT] + [VMEM] * 3 + [WEIGHT] * 3,
        [shaped(n, F32), shaped(n, F32)] + [shaped(slots, F32)] * ACCS,
        "edge_message",
    )(*index, senders.reshape(-1, 128), pre, edges, ghosts, w_in, w_out, gain)


def node_update(rows, kept, first, second, w_in, w_out, gain, level):
    count, width = rows.shape
    n = min(512, count)

    def kernel(rows_ref, kept_ref, first_ref, second_ref, w_late, wo_late, gain_late, out_ref):
        for late in (w_late, wo_late, gain_late):
            late.wait()
        w_n = w_late.ref[level, 0:width, :]
        w_a = w_late.ref[level, width : 2 * width, :]
        w_o = wo_late.ref[level]
        scale = gain_late.ref[level : level + 1, :]

        def step(at):
            own = rows_ref[pl.ds(at, n), :]
            total = (
                kept_ref[pl.ds(at, n), :]
                + first_ref[pl.ds(at, n), :].astype(F32)
                + second_ref[pl.ds(at, n), :].astype(F32)
            ).astype(BF)
            hidden = silu(dot(own, w_n) + dot(total, w_a)).astype(BF)
            result = norm(dot(hidden, w_o), scale)
            out_ref[pl.ds(at, n), :] = (own.astype(F32) + result).astype(BF)

        blocks(count, n, step)

    return call(kernel, shaped(count, BF), [VMEM] * 4 + [WEIGHT] * 3, (), "node_update")(
        rows, kept, first, second, w_in, w_out, gain
    )


def take_rows(tables, index):
    width = tables[0].shape[1]
    rows = sum(x.shape[0] for x in tables)
    count = index.shape[0]

    def kernel(index_late, *refs):
        refs, (out_ref, wide, picked) = refs[:-3], refs[-3:]
        start = 0
        for ref in refs:

            def widen(at, ref=ref, start=start):
                wide[pl.ds(start + at, 256), :] = ref[pl.ds(at, 256), :].astype(F32)

            blocks(ref.shape[0], 256, widen)
            start += ref.shape[0]
        index_late.wait()

        def gather(i, carry):
            base = i * UNROLL
            for j in range(UNROLL):
                picked[pl.ds(base + j, 1), :] = wide[pl.ds(index_late.ref[base + j], 1), :]
            return carry

        lax.fori_loop(0, count // UNROLL, gather, 0)

        def narrow(at):
            out_ref[pl.ds(at, 256), :] = picked[pl.ds(at, 256), :].astype(BF)

        blocks(count, 256, narrow)

    return call(
        kernel,
        shaped(count, BF),
        [INDEX] + [VMEM] * len(tables),
        [shaped(rows, F32), shaped(count, F32)],
        "take_rows",
    )(index, *tables)


def resolve(table, index):
    count = index.shape[0]

    def kernel(table_late, index_late, out_ref):
        table_late.wait()
        index_late.wait()

        def look(i, carry):
            base = i * UNROLL
            for j in range(UNROLL):
                out_ref[base + j] = table_late.ref[index_late.ref[base + j]]
            return carry

        lax.fori_loop(0, count // UNROLL, look, 0)

    return call(kernel, jax.ShapeDtypeStruct((count,), jnp.int32), [INDEX, INDEX], (), "resolve")(table, index)


def pool_sum(arrived, places):
    count, width = arrived.shape
    n = 256

    def kernel(arrived_ref, places_late, out_ref):
        places_late.wait()
        rows = arrived_ref[...]

        def step(at):
            pick = (places_late.ref[...] == at + lax.broadcasted_iota(jnp.int32, (n, count), 0)).astype(BF)
            out_ref[pl.ds(at, n), :] = dot(pick, rows)

        blocks(COARSE, n, step)

    return call(kernel, shaped(COARSE, F32), [VMEM, WEIGHT], (), "pool_sum")(arrived, places.reshape(1, count))


def child_count(places):
    count = places.shape[0]
    high = (places // 128)[None, :] == jnp.arange(COARSE // 128, dtype=jnp.int32)[:, None]
    low = (places % 128)[:, None] == jnp.arange(128, dtype=jnp.int32)[None, :]
    return dot(high.astype(BF), low.astype(BF)).reshape(COARSE)


def swap(x, bit):
    size = lax.axis_size("edge")
    return lax.ppermute(x, "edge", [(i, i ^ bit) for i in range(size)])


def layer_sums(nodes, edges, senders, receivers, border, level, w, slots, table):
    rows, width = nodes.shape
    outgoing = nodes[border[0].reshape(-1)].reshape(border.shape[1], border.shape[2], width)
    arrived = lax.all_to_all(outgoing, "dom", split_axis=0, concat_axis=0, tiled=True)
    ghosts = arrived.reshape(-1, width)
    pre = edge_gather(nodes, senders, receivers, w[0], level, ghosts.shape[0])
    if table is None:
        me = lax.axis_index("edge")
        quarter = rows // 4
        receivers = order_of((receivers // quarter) ^ me) * quarter + receivers % quarter
    k0, k2, s1, s3 = edge_message(
        pre, edges, ghosts, senders, receivers, table, w[0], w[1], w[4], level, rows, slots
    )
    second = swap((k2 + swap(s3, 1).astype(F32)).astype(BF), 2)
    return k0, swap(s1, 1), second


def order_of(rel):
    return (rel & 1) * 2 + (rel >> 1)


def shards(
    fine_nodes,
    fine_edges,
    fine_senders,
    fine_receivers,
    fine_halo,
    coarse_edges,
    coarse_senders,
    coarse_receivers,
    coarse_halo,
    pool_send,
    pool_dest,
    unpool_slot,
    edge_in_weight,
    edge_out_weight,
    node_in_weight,
    node_out_weight,
    edge_gain,
    node_gain,
):
    w = (edge_in_weight, edge_out_weight, node_in_weight, node_out_weight, edge_gain, node_gain)
    width = fine_nodes.shape[-1]
    n_dom = pool_send.shape[1]
    span = pool_send.shape[2]
    part = span // 4
    slots = n_dom * span
    quarter = n_dom * part
    me = lax.axis_index("edge")
    target = unpool_slot // span
    within = unpool_slot % span
    slot_place = order_of((within // part) ^ me) * quarter + target * part + within % part
    my_send = lax.dynamic_slice_in_dim(pool_send[0], me * part, part, 1).reshape(-1)
    my_dest = lax.dynamic_slice_in_dim(pool_dest[0], me * part, part, 1).reshape(-1)
    counts = child_count(pool_dest[0].reshape(-1))
    scale = jnp.maximum(counts, 1.0)[:, None]

    kept, first, second = layer_sums(
        fine_nodes, fine_edges, fine_senders, fine_receivers, fine_halo, 0, w, slots, slot_place
    )
    direct = n_dom == 8
    my_send, lists, kept = lax.optimization_barrier((my_send, pool_dest[0], kept))
    if direct:
        known = lax.all_to_all(lists, "dom", 0, 0, tiled=True)
        place = place_of(known)
    own = take_rows([fine_nodes], my_send)
    mid = node_update(own, kept, first, second, w[2], w[3], w[5], 0)

    arrived = lax.all_to_all(mid.reshape(n_dom, part, width), "dom", split_axis=0, concat_axis=0, tiled=True)
    if direct:
        mid_x = swap(mid, 2)
        place, slot_of, _ = lax.optimization_barrier((place, unpool_slot, mid))
        parent = resolve(place, slot_of)
        my_dest, parent, arrived, mid_x = lax.optimization_barrier((my_dest, parent, arrived, mid_x))
    sums = pool_sum(arrived.reshape(-1, width), my_dest)
    bit = me & 1
    half = COARSE // 2
    mine = lax.dynamic_slice_in_dim(sums, bit * half, half, 0)
    theirs = lax.dynamic_slice_in_dim(sums, (1 - bit) * half, half, 0)
    mine = mine + swap(theirs, 1)
    mine = mine + swap(mine.astype(BF), 2).astype(F32)
    mine = (mine / lax.dynamic_slice_in_dim(scale, bit * half, half, 0)).astype(BF)
    if direct:
        mine, mid, mid_1, mid_3 = lax.optimization_barrier((mine, mid, swap(mid, 1), swap(mid_x, 1)))
    theirs = swap(mine, 1)
    coarse_in = jnp.concatenate([jnp.where(bit == 0, mine, theirs), jnp.where(bit == 0, theirs, mine)], axis=0)

    kept, first, second = layer_sums(
        coarse_in, coarse_edges, coarse_senders, coarse_receivers, coarse_halo, 1, w, COARSE, None
    )
    fourth = COARSE // 4
    own = lax.dynamic_slice_in_dim(coarse_in, me * fourth, fourth, 0)
    top = node_update(own, kept, first, second, w[2], w[3], w[5], 1)
    if direct:
        return spread_out(top, [mid, mid_x, mid_1, mid_3], slot_place, parent)

    coarse_out = lax.all_gather(top, "edge", axis=0, tiled=True)
    parents = take_rows([coarse_out], jnp.minimum(my_dest, COARSE - 1))
    back = lax.all_to_all(parents.reshape(n_dom, part, width), "dom", split_axis=0, concat_axis=0, tiled=True)
    final = (mid.astype(F32) + back.reshape(-1, width).astype(F32)).astype(BF)
    final_x = swap(final, 2)
    fine_out = take_rows([final, final_x, swap(final, 1), swap(final_x, 1)], slot_place)
    return (fine_out, coarse_out)


def place_of(known):
    me = lax.axis_index("edge")
    here = lax.axis_index("dom")
    fourth = COARSE // 4
    owner = jnp.arange(known.shape[0], dtype=jnp.int32)[:, None]
    rel = (known // fourth) ^ me
    spot = (rel & 1) * 4 + (rel >> 1) * 2 + ((owner ^ here) & 1)
    return (spot * (4 * fourth) + (owner >> 1) * fourth + known % fourth).reshape(-1)


def spread_out(top, mids, slot_place, parent):
    fourth, width = top.shape
    me = lax.axis_index("edge")
    here = lax.axis_index("dom")
    lines = [[0, 2, 4, 6], [1, 3, 5, 7]]

    def cross(x):
        return lax.ppermute(x, "dom", [(i, i ^ 1) for i in range(8)])

    copies = jnp.broadcast_to(top[None], (4, fourth, width))
    line = lax.all_to_all(copies, "dom", 0, 0, tiled=True, axis_index_groups=lines).reshape(4 * fourth, width)
    slot_place, _ = lax.optimization_barrier((slot_place, top))
    mid_rows = take_rows(mids, slot_place)
    line, mid_rows = lax.optimization_barrier((line, mid_rows))
    line_y = cross(line)
    line_x = swap(line, 2)
    corner_x = swap(line_y[: 2 * fourth], 2)
    corner_y = cross(line_x[2 * fourth :])
    pieces = [line, line_y, line_x, corner_x, corner_y]
    pieces = pieces + [swap(x, 1) for x in pieces]

    rel = jnp.arange(4, dtype=jnp.int32) ^ me
    starts = ((rel & 1) * 4 + (rel >> 1) * 2) * (4 * fourth) + (here >> 1) * fourth
    return unpool(pieces, mid_rows, parent, starts)


def unpool(pieces, mid_rows, parent, starts):
    count, width = mid_rows.shape
    total = sum(x.shape[0] for x in pieces)
    fourth = COARSE // 4

    def kernel(parent_ref, starts_ref, mid_ref, *refs):
        refs, (out_ref, coarse_ref, wide, picked) = refs[:-4], refs[-4:]
        start = 0
        for ref in refs:

            def widen(at, ref=ref, start=start):
                wide[pl.ds(start + at, 256), :] = ref[pl.ds(at, 256), :].astype(F32)

            blocks(ref.shape[0], 256, widen)
            start += ref.shape[0]
        parent_ref.wait()

        def gather(i, carry):
            base = i * UNROLL
            for j in range(UNROLL):
                picked[pl.ds(base + j, 1), :] = wide[pl.ds(parent_ref.ref[base + j], 1), :]
            return carry

        lax.fori_loop(0, count // UNROLL, gather, 0)
        starts_ref.wait()
        for k in range(4):
            rows = wide[pl.ds(pl.multiple_of(starts_ref.ref[k], fourth), fourth), :]
            coarse_ref[k * fourth : (k + 1) * fourth, :] = rows.astype(BF)

        def narrow(at):
            out_ref[pl.ds(at, 256), :] = (picked[pl.ds(at, 256), :] + mid_ref[pl.ds(at, 256), :].astype(F32)).astype(BF)

        blocks(count, 256, narrow)

    return call(
        kernel,
        (shaped(count, BF), shaped(COARSE, BF)),
        [INDEX, INDEX, VMEM] + [VMEM] * len(pieces),
        [shaped(total, F32), shaped(count, F32)],
        "unpool",
    )(parent, starts, mid_rows, *pieces)


def solution(mesh):
    placed = (
        P("dom", None),
        P(("dom", "edge"), None),
        P(("dom", "edge")),
        P(("dom", "edge")),
        P("dom", None, None),
        P(("dom", "edge"), None),
        P(("dom", "edge")),
        P(("dom", "edge")),
        P("dom", None, None),
        P("dom", None, None),
        P("dom", None, None),
        P("dom"),
        P(),
        P(),
        P(),
        P(),
        P(),
        P(),
    )
    return jax.shard_map(
        shards,
        mesh=mesh,
        in_specs=placed,
        out_specs=(P("dom", None), P("dom", None)),
        check_vma=False,
    )
```

```python
import jax
import jax.numpy as jnp
from jax import lax
from jax.experimental import pallas as pl
from jax.experimental.pallas import tpu as pltpu
from jax.sharding import PartitionSpec as P


BF = jnp.bfloat16
F32 = jnp.float32
VMEM = pl.BlockSpec(memory_space=pltpu.VMEM)
SMEM = pl.BlockSpec(memory_space=pltpu.SMEM)
HBM = pl.BlockSpec(memory_space=pltpu.HBM)
INDEX = "index"
WEIGHT = "weight"
LOAD = "load"
LATE = (INDEX, WEIGHT, LOAD)
FULL = 60 * 1024 * 1024
COARSE = 2048
UNROLL = 32
ACCS = 4
CHUNKS = 1


def nbytes(x):
    width = -(-x.shape[-1] // 128) * 128
    return x.size // x.shape[-1] * width * x.dtype.itemsize


class Late:
    def __init__(self, source, ref, sems):
        self.ref = ref
        self.pieces = sems.shape[0]
        self.size = source.shape[0] // self.pieces
        self.copies = []
        for k in range(self.pieces):
            at = pl.ds(k * self.size, self.size)
            self.copies.append(pltpu.make_async_copy(source.at[at], ref.at[at], sems.at[k]))
            self.copies[-1].start()

    def wait(self):
        for copy in self.copies:
            copy.wait()

    def loop(self, body, unroll, after=None):
        for k, copy in enumerate(self.copies):
            copy.wait()

            def step(i, carry, start=k * self.size):
                for j in range(unroll):
                    body(start + i * unroll + j)
                return carry

            lax.fori_loop(0, self.size // unroll, step, 0)
            if after is not None:
                after(k, self.size)


def pieces_of(x, spec):
    return x.shape[0] // 2048 if spec in (INDEX, LOAD) and x.shape[0] % 2048 == 0 else 1


def call(kernel, out_shape, in_specs, scratch=(), out_specs=None, full=False):
    def run(*args):
        late = [k for k, spec in enumerate(in_specs) if spec in LATE]
        homes = [(pltpu.SMEM if in_specs[k] is INDEX else pltpu.VMEM)(args[k].shape, args[k].dtype) for k in late]
        sems = [pltpu.SemaphoreType.DMA((pieces_of(args[k], in_specs[k]),)) for k in late]
        used = sum(nbytes(x) for x, spec in zip(args, in_specs) if spec is not INDEX)
        used += sum(nbytes(x) for x in jax.tree.leaves(out_shape))
        used += sum(nbytes(x) for x in scratch if hasattr(x, "size"))
        n_out = len(jax.tree.leaves(out_shape))

        def body(*refs):
            ins, outs = list(refs[: len(args)]), refs[len(args) : len(args) + n_out]
            mine = refs[len(args) + n_out : len(args) + n_out + len(scratch)]
            rest = refs[len(args) + n_out + len(scratch) :]
            for at, k in enumerate(late):
                ins[k] = Late(ins[k], rest[at], rest[len(late) + at])
            kernel(*ins, *outs, *mine)

        return pl.pallas_call(
            body,
            out_shape=out_shape,
            in_specs=[HBM if spec in LATE else spec for spec in in_specs],
            out_specs=out_specs or jax.tree.map(lambda x: VMEM, out_shape),
            scratch_shapes=[pltpu.VMEM(x.shape, x.dtype) if hasattr(x, "size") else x for x in scratch]
            + homes
            + sems,
            compiler_params=pltpu.CompilerParams(vmem_limit_bytes=FULL if full else used + 2 * 1024 * 1024),
        )(*args)

    return run


def shaped(rows, dtype, width=128):
    return jax.ShapeDtypeStruct((rows, width), dtype)


def dot(a, b):
    return jnp.dot(a, b, preferred_element_type=F32)


def silu(v):
    return v / (1.0 + jnp.exp(-v))


def norm(values, gain):
    center = values - jnp.mean(values, axis=-1, keepdims=True)
    spread = jnp.mean(center * center, axis=-1, keepdims=True)
    return center * lax.rsqrt(spread + 1e-05) * gain


def chunk(total, size):
    return max(k for k in range(16, min(size, total) + 1, 16) if total % k == 0)


def blocks(total, size, body):
    size = min(size, total)

    def step(i, carry):
        body(pl.multiple_of(i * size, size))
        return carry

    lax.fori_loop(0, total // size, step, 0)


def edge_gather(nodes, senders, receivers, table, w_in, level, ghost_rows):
    rows, width = nodes.shape
    count = senders.shape[0]
    mapped = table is not None
    n = 128

    def kernel(send_idx, recv_idx, w_late, nodes_late, *refs):
        if mapped:
            table_late, lines_late, refs = refs[0], refs[1], refs[2:]
            out_ref, place_ref, send_tab, recv_tab, stage, places, sems = refs
        else:
            out_ref, send_tab, recv_tab, stage, sems = refs
        send_tab[pl.ds(rows, ghost_rows), :] = jnp.zeros((ghost_rows, width), F32)
        w_late.wait()
        w_s = w_late.ref[level, 0:width, :]
        w_r = w_late.ref[level, width : 2 * width, :]
        for k, copy in enumerate(nodes_late.copies):
            copy.wait()

            def project(at, start=k * nodes_late.size):
                block = nodes_late.ref[pl.ds(start + at, 512), :]
                send_tab[pl.ds(start + at, 512), :] = dot(block, w_s)
                recv_tab[pl.ds(start + at, 512), :] = dot(block, w_r)

            blocks(nodes_late.size, 512, project)
        if mapped:
            table_late.wait()
            lines_late.wait()
            high, low = digits(table_late.ref[...])
        send_idx.wait()
        copies = []
        for k, copy in enumerate(recv_idx.copies):
            copy.wait()
            start = k * recv_idx.size

            def gather(i, carry, start=start):
                base = start + i * n
                for j in range(n):
                    s = send_idx.ref[base + j]
                    r = recv_idx.ref[base + j]
                    stage[pl.ds(base + j, 1), :] = send_tab[pl.ds(s, 1), :] + recv_tab[pl.ds(r, 1), :]
                if mapped:
                    line = pl.ds(start // n + i, 1)
                    places[line, :] = look_up(high, low, lines_late.ref[line, :])
                return carry

            lax.fori_loop(0, recv_idx.size // n, gather, 0)
            spot = pl.ds(start, recv_idx.size)
            copies.append(pltpu.make_async_copy(stage.at[spot], out_ref.at[spot], sems.at[k]))
            copies[-1].start()
        if mapped:
            copies.append(pltpu.make_async_copy(places, place_ref, sems.at[recv_idx.pieces]))
            copies[-1].start()
        for copy in copies:
            copy.wait()

    any_space = pl.BlockSpec(memory_space=pl.ANY)
    sems = pltpu.SemaphoreType.DMA((pieces_of(receivers, INDEX) + 1,))
    scratch = [shaped(rows + ghost_rows, F32), shaped(rows, F32), shaped(count, F32)]
    args = (senders, receivers, w_in, nodes)
    specs = [INDEX, INDEX, WEIGHT, LOAD]
    if not mapped:
        return call(kernel, shaped(count, F32), specs, scratch + [sems], any_space, level == 0)(*args), None
    places = shaped(count // n, jnp.int32)
    pre, place = call(
        kernel,
        (shaped(count, F32), places),
        specs + [WEIGHT, WEIGHT],
        scratch + [places, sems],
        (any_space, any_space),
        True,
    )(*args, table.reshape(-1, 128), receivers.reshape(-1, 128))
    return pre, place.reshape(-1)


def edge_message(pre, edges, ghosts, senders, places, w_in, w_out, gain, level, rows, slots):
    count, width = pre.shape
    ghost_rows = ghosts.shape[0]
    fourth = slots // 4
    n = 256
    total = count // n

    def kernel(recv_idx, *refs):
        (send_late, w_late, wo_late, gain_late, pre_late, edge_late, ghost_late,
         k0_ref, k2_ref, s1_ref, s3_ref, even, odd, k0_st, k2_st, s1_st, s3_st) = refs[:17]
        accs, sems = refs[17:-1], refs[-1]

        room = chunk(slots, 512)

        def clear(at):
            for acc in accs:
                acc[pl.ds(at, room), :] = jnp.zeros((room, width), F32)

        blocks(slots, room, clear)
        send_late.wait()
        w_late.wait()
        wo_late.wait()
        gain_late.wait()
        pre_late.wait()
        edge_late.wait()
        ghost_late.wait()
        w_s = w_late.ref[level, 0:width, :]
        w_e = w_late.ref[level, 2 * width : 3 * width, :]
        w_o = wo_late.ref[level]
        scale = gain_late.ref[level : level + 1, :]

        def message(b, msg):
            at = pl.multiple_of(b * n, n)
            columns = []
            for k in range(n // 128):
                far = (send_late.ref[pl.ds(b * (n // 128) + k, 1), :] - rows).astype(F32)
                columns.append(jnp.broadcast_to(far, (8, 128)).T[:, 0:1])
            column = jnp.concatenate(columns, axis=0)
            lane = lax.broadcasted_iota(jnp.int32, (n, ghost_rows), 1).astype(F32)
            pick = (column == lane).astype(BF)
            picked = dot(pick, ghost_late.ref[...]).astype(BF)
            first = pre_late.ref[pl.ds(at, n), :] + (dot(picked, w_s) + dot(edge_late.ref[pl.ds(at, n), :], w_e))
            msg[...] = norm(dot(silu(first).astype(BF), w_o), scale)

        def scatter(b, msg):
            base = b * n
            for j in range(n):
                acc = accs[j % ACCS]
                r = recv_idx.ref[base + j]
                acc[pl.ds(r, 1), :] = acc[pl.ds(r, 1), :] + msg[pl.ds(j, 1), :]

        message(0, even)
        recv_idx.wait()

        def step(i, carry):
            b = 2 * i
            message(b + 1, odd)
            scatter(b, even)
            message(jnp.minimum(b + 2, total - 1), even)
            scatter(b + 1, odd)
            return carry

        lax.fori_loop(0, total // 2, step, 0)
        copies = []
        outs = ((3, s3_st, s3_ref), (1, k2_st, k2_ref), (2, s1_st, s1_ref), (0, k0_st, k0_ref))
        for k, (place, stage, out_ref) in enumerate(outs):
            m = chunk(fourth, 400)

            def body(at, stage=stage, start=place * fourth, m=m):
                value = accs[0][pl.ds(at + start, m), :]
                for acc in accs[1:]:
                    value = value + acc[pl.ds(at + start, m), :]
                stage[pl.ds(at, m), :] = value.astype(stage.dtype)

            blocks(fourth, m, body)
            copies.append(pltpu.make_async_copy(stage, out_ref, sems.at[k]))
            copies[-1].start()
        for copy in copies:
            copy.wait()

    outs = (shaped(fourth, F32), shaped(fourth, F32), shaped(fourth, BF), shaped(fourth, BF))
    return call(
        kernel,
        outs,
        [INDEX] + [WEIGHT] * 4 + [LOAD] * 3,
        [shaped(n, F32), shaped(n, F32), *outs]
        + [shaped(slots, F32)] * ACCS
        + [pltpu.SemaphoreType.DMA((4,))],
        (pl.BlockSpec(memory_space=pl.ANY),) * 4,
        level == 0,
    )(places, senders.reshape(-1, 128), w_in, w_out, gain, pre, edges, ghosts)


def node_update(rows, kept, first, second, w_in, w_out, gain, level):
    count, width = rows.shape
    n = chunk(count, 704)

    def kernel(rows_ref, kept_ref, first_ref, second_ref, w_ref, wo_ref, gain_ref, out_ref):
        own = rows_ref[...]
        total = (kept_ref[...] + first_ref[...].astype(F32) + second_ref[...].astype(F32)).astype(BF)
        hidden = silu(dot(own, w_ref[level, 0:width, :]) + dot(total, w_ref[level, width : 2 * width, :])).astype(BF)
        result = norm(dot(hidden, wo_ref[level]), gain_ref[level : level + 1, :])
        out_ref[...] = (own.astype(F32) + result).astype(BF)

    block = pl.BlockSpec((n, width), lambda i: (i, 0))
    return pl.pallas_call(
        kernel,
        grid=(count // n,),
        out_shape=shaped(count, BF),
        in_specs=[block] * 4
        + [pl.BlockSpec(x.shape, lambda i, d=x.ndim: (0,) * d) for x in (w_in, w_out, gain)],
        out_specs=block,
        name="node_update",
        compiler_params=pltpu.CompilerParams(vmem_limit_bytes=FULL if level == 0 else 8 * 1024 * 1024),
    )(rows, kept, first, second, w_in, w_out, gain)


def take_rows(tables, index):
    rows = sum(x.shape[0] for x in tables)
    count = index.shape[0]

    def kernel(index_late, *refs):
        refs, (out_ref, wide, picked) = refs[:-3], refs[-3:]
        start = 0
        for ref in refs:

            m = chunk(ref.shape[0], 400)

            def widen(at, ref=ref, start=start, m=m):
                wide[pl.ds(start + at, m), :] = ref[pl.ds(at, m), :].astype(F32)

            blocks(ref.shape[0], m, widen)
            start += ref.shape[0]

        def gather(j):
            picked[pl.ds(j, 1), :] = wide[pl.ds(index_late.ref[j], 1), :]

        index_late.loop(gather, UNROLL)

        def narrow(at):
            out_ref[pl.ds(at, 256), :] = picked[pl.ds(at, 256), :].astype(BF)

        blocks(count, 256, narrow)

    return call(
        kernel, shaped(count, BF), [INDEX] + [VMEM] * len(tables), [shaped(rows, F32), shaped(count, F32)]
    )(index, *tables)


def packed_rows(nodes, index, base, room):
    rows, width = nodes.shape
    n_dom, part = index.shape
    unroll = chunk(part, 32)

    def kernel(base_late, index_late, nodes_ref, out_ref, wide, picked):
        m = chunk(room + part, 512)

        def clear(at):
            picked[pl.ds(at, m), :] = jnp.zeros((m, width), F32)

        blocks(room + part, m, clear)

        def widen(at):
            wide[pl.ds(at, 256), :] = nodes_ref[pl.ds(at, 256), :].astype(F32)

        blocks(rows, 256, widen)
        base_late.wait()
        index_late.wait()

        def group(p, carry):
            start = base_late.ref[p]

            def gather(i, c):
                at = i * unroll
                for j in range(unroll):
                    picked[pl.ds(start + at + j, 1), :] = wide[pl.ds(index_late.ref[p * part + at + j], 1), :]
                return c

            return lax.fori_loop(0, part // unroll, gather, carry)

        lax.fori_loop(0, n_dom, group, 0)
        m = chunk(room, 400)

        def narrow(at, m=m):
            out_ref[pl.ds(at, m), :] = picked[pl.ds(at, m), :].astype(BF)

        blocks(room, m, narrow)

    return call(
        kernel, shaped(room, BF), [INDEX, INDEX, VMEM], [shaped(rows, F32), shaped(room + part, F32)]
    )(base, index.reshape(-1), nodes)


def expand(packed, base, part):
    room, width = packed.shape
    n_dom = base.shape[0]

    def kernel(base_late, packed_ref, out_ref, wide):
        wide[pl.ds(room, part), :] = jnp.zeros((part, width), F32)
        m = chunk(room, 400)

        def widen(at):
            wide[pl.ds(at, m), :] = packed_ref[pl.ds(at, m), :].astype(F32)

        blocks(room, m, widen)
        base_late.wait()

        def copy(p, carry):
            rows = wide[pl.ds(base_late.ref[p], part), :]
            out_ref[pl.ds(pl.multiple_of(p * part, 16), part), :] = rows.astype(BF)
            return carry

        lax.fori_loop(0, n_dom, copy, 0)

    return call(kernel, shaped(n_dom * part, BF), [INDEX, VMEM], [shaped(room + part, F32)])(base, packed)


def layout(unpool_slot, me, n_dom, span, room):
    lines = unpool_slot.shape[0] // 128

    def kernel(me_ref, slot_ref, place_ref, base_ref):
        here = me_ref[0]
        slot = slot_ref[...]
        owner = jnp.zeros_like(slot)
        for k in range(1, n_dom):
            owner = owner + (slot >= k * span).astype(jnp.int32)
        within = slot - owner * span
        quarter = within & 3
        place = jnp.zeros_like(slot)
        starts = [jnp.int32(0)] * 4
        for k in range(n_dom):
            mine = owner == k
            count = jnp.sum(mine.astype(F32)).astype(jnp.int32)
            base = jnp.int32(0)
            for e in range(4):
                place = jnp.where(mine & (quarter == e), starts[e], place)
                base = base + jnp.where(here == e, starts[e], 0)
                starts[e] = starts[e] + ((count - e + 3) >> 2)
            base_ref[k] = base
        rel = quarter ^ here
        place_ref[...] = ((rel & 1) * 2 + (rel >> 1)) * room + place + (within >> 2)

    place, base = pl.pallas_call(
        kernel,
        out_shape=(jax.ShapeDtypeStruct((lines, 128), jnp.int32), jax.ShapeDtypeStruct((n_dom,), jnp.int32)),
        in_specs=[SMEM, VMEM],
        out_specs=(VMEM, SMEM),
        name="layout",
        compiler_params=pltpu.CompilerParams(vmem_limit_bytes=8 * 1024 * 1024),
    )(me.reshape(1), unpool_slot.reshape(lines, 128))
    return place.reshape(-1), base


def digits(table):
    return (table >> 7).astype(F32).T.astype(BF), (table & 127).astype(F32).T.astype(BF)


def look_up(high, low, at):
    pick = (lax.broadcasted_iota(jnp.int32, (high.shape[1], 128), 0) == (at >> 7)).astype(BF)
    value = dot(high, pick) * 128.0 + dot(low, pick)
    lane = lax.broadcasted_iota(jnp.int32, (128, 128), 0) == (at & 127)
    return jnp.sum(jnp.where(lane, value, 0.0), axis=0, keepdims=True).astype(jnp.int32)


def resolve(table, index):
    lines = index.shape[0] // 128
    tall = table.shape[0] // 128

    def kernel(table_ref, index_ref, out_ref):
        high, low = digits(table_ref[...])

        def step(i, carry):
            for k in range(8):
                out_ref[pl.ds(i * 8 + k, 1), :] = look_up(high, low, index_ref[pl.ds(i * 8 + k, 1), :])
            return carry

        lax.fori_loop(0, lines // 8, step, 0)

    out = jax.ShapeDtypeStruct((lines, 128), jnp.int32)
    return call(kernel, out, [VMEM, VMEM], ())(table.reshape(tall, 128), index.reshape(lines, 128)).reshape(-1)


def pool_sum(arrived, places, bit):
    count, _ = arrived.shape
    n = 256
    half = COARSE // 2

    def kernel(bit_late, arrived_ref, places_late, mine_ref, theirs_ref):
        places_late.wait()
        bit_late.wait()
        rows = arrived_ref[...]
        for out_ref, start in ((theirs_ref, (1 - bit_late.ref[0]) * half), (mine_ref, bit_late.ref[0] * half)):

            def step(at, out_ref=out_ref, start=start):
                near = jnp.clip(places_late.ref[...] - (start + at), -1, n).astype(F32).astype(BF)
                row = lax.broadcasted_iota(jnp.int32, (n, count), 0).astype(F32).astype(BF)
                pick = jnp.where(near == row, jnp.ones((), BF), jnp.zeros((), BF))
                out_ref[pl.ds(at, n), :] = dot(pick, rows)

            blocks(half, n, step)

    return call(kernel, (shaped(half, F32), shaped(half, F32)), [INDEX, VMEM, WEIGHT], ())(
        bit.reshape(1), arrived, places.reshape(1, count)
    )


def child_count(places):
    high = (places // 128)[None, :] == jnp.arange(COARSE // 128, dtype=jnp.int32)[:, None]
    low = (places % 128)[:, None] == jnp.arange(128, dtype=jnp.int32)[None, :]
    return dot(high.astype(BF), low.astype(BF)).reshape(COARSE)


def swap(x, bit):
    size = lax.axis_size("edge")
    return lax.ppermute(x, "edge", [(i, i ^ bit) for i in range(size)])


def layer_sums(nodes, edges, senders, receivers, border, level, w, slots, table):
    rows, width = nodes.shape
    outgoing = nodes[border[0].reshape(-1)].reshape(border.shape[1], border.shape[2], width)
    arrived = lax.all_to_all(outgoing, "dom", split_axis=0, concat_axis=0, tiled=True)
    ghosts = arrived.reshape(-1, width)
    pre, places = edge_gather(nodes, senders, receivers, table, w[0], level, ghosts.shape[0])
    if table is None:
        me = lax.axis_index("edge")
        quarter = rows // 4
        places = order_of((receivers // quarter) ^ me) * quarter + receivers % quarter
    k0, k2, s1, s3 = edge_message(pre, edges, ghosts, senders, places, w[0], w[1], w[4], level, rows, slots)
    second = swap((k2 + swap(s3, 1).astype(F32)).astype(BF), 2)
    return k0, swap(s1, 1), second


def order_of(rel):
    return (rel & 1) * 2 + (rel >> 1)


def shards(
    fine_nodes,
    fine_edges,
    fine_senders,
    fine_receivers,
    fine_halo,
    coarse_edges,
    coarse_senders,
    coarse_receivers,
    coarse_halo,
    pool_send,
    pool_dest,
    unpool_slot,
    edge_in_weight,
    edge_out_weight,
    node_in_weight,
    node_out_weight,
    edge_gain,
    node_gain,
):
    w = (edge_in_weight, edge_out_weight, node_in_weight, node_out_weight, edge_gain, node_gain)
    width = fine_nodes.shape[-1]
    n_dom = pool_send.shape[1]
    span = pool_send.shape[2]
    part = span // 4
    me = lax.axis_index("edge")
    direct = n_dom == 8
    room = -(-(fine_nodes.shape[0] // 4 + n_dom) // 64) * 64
    slot_place, base = layout(unpool_slot, me, n_dom, span, room)

    def own_quarter(lists):
        return lax.dynamic_index_in_dim(lists[0].reshape(n_dom, part, 4), me, 2, keepdims=False)

    my_dest = own_quarter(pool_dest).reshape(-1)
    counts = child_count(pool_dest[0].reshape(-1))
    scale = jnp.maximum(counts, 1.0)[:, None]

    kept, first, second = layer_sums(
        fine_nodes, fine_edges, fine_senders, fine_receivers, fine_halo, 0, w, 4 * room, slot_place
    )
    sends, kept = lax.optimization_barrier((pool_send, kept))
    own = packed_rows(fine_nodes, own_quarter(sends), base, room)
    mid = node_update(own, kept, first, second, w[2], w[3], w[5], 0)
    if direct:
        mid_x = swap(mid, 2)
    spread = expand(mid, base, part)
    arrived = lax.all_to_all(spread.reshape(n_dom, part, width), "dom", split_axis=0, concat_axis=0, tiled=True)
    bit = me & 1
    half = COARSE // 2
    mine, theirs = pool_sum(arrived.reshape(-1, width), my_dest, bit)
    mine = mine + swap(theirs, 1)
    half_sum = mine.astype(BF)
    if direct:
        lists, half_sum = lax.optimization_barrier((pool_dest[0], half_sum))
    other = swap(half_sum, 2)
    if direct:
        known = lax.all_to_all(lists, "dom", 0, 0, tiled=True)
    mine = mine + other.astype(F32)
    mine = (mine / lax.dynamic_slice_in_dim(scale, bit * half, half, 0)).astype(BF)
    if direct:
        mine, mid, mid_1, mid_3, known = lax.optimization_barrier((mine, mid, swap(mid, 1), swap(mid_x, 1), known))
    theirs = swap(mine, 1)
    coarse_in = jnp.concatenate([jnp.where(bit == 0, mine, theirs), jnp.where(bit == 0, theirs, mine)], axis=0)

    kept, first, second = layer_sums(
        coarse_in, coarse_edges, coarse_senders, coarse_receivers, coarse_halo, 1, w, COARSE, None
    )
    fourth = COARSE // 4
    own = lax.dynamic_slice_in_dim(coarse_in, me * fourth, fourth, 0)
    top = node_update(own, kept, first, second, w[2], w[3], w[5], 1)
    if direct:
        return spread_out(top, [mid, mid_x, mid_1, mid_3], slot_place, known, unpool_slot)

    coarse_out = lax.all_gather(top, "edge", axis=0, tiled=True)
    parents = take_rows([coarse_out], jnp.minimum(my_dest, COARSE - 1))
    back = lax.all_to_all(parents.reshape(n_dom, part, width), "dom", split_axis=0, concat_axis=0, tiled=True)
    final = (spread.astype(F32) + back.reshape(-1, width).astype(F32)).astype(BF)
    final_x = swap(final, 2)
    within = unpool_slot % span
    place = order_of((within % 4) ^ me) * (n_dom * part) + (unpool_slot // span) * part + within // 4
    fine_out = take_rows([final, final_x, swap(final, 1), swap(final_x, 1)], place)
    return (fine_out, coarse_out)


def spot_of(rel, dy, z, row):
    fourth = COARSE // 4
    size = fourth // CHUNKS
    return (rel & 1) * (16 * fourth) + (row // size) * (16 * size) + ((rel >> 1) * 2 + dy) * (4 * size) + z * size + row % size


def place_of(known):
    me = lax.axis_index("edge")
    here = lax.axis_index("dom")
    fourth = COARSE // 4
    owner = jnp.arange(known.shape[0], dtype=jnp.int32).reshape((-1,) + (1,) * (known.ndim - 1))
    return spot_of((known // fourth) ^ me, (owner ^ here) & 1, owner >> 1, known % fourth).reshape(-1)


def spread_out(top, mids, slot_place, known, unpool_slot):
    fourth, width = top.shape
    size = fourth // CHUNKS
    me = lax.axis_index("edge")
    here = lax.axis_index("dom")
    groups = [[0, 2, 4, 6], [1, 3, 5, 7]]

    def cross(x):
        return lax.ppermute(x, "dom", [(i, i ^ 1) for i in range(8)])

    slot_place, known, _ = lax.optimization_barrier((slot_place, known, top))
    parent = resolve(place_of(known), unpool_slot)
    mid_rows = take_rows(mids, slot_place)
    lines = []
    for h in range(CHUNKS):
        copies = jnp.broadcast_to(top[None, h * size : (h + 1) * size], (4, size, width))
        line = lax.all_to_all(copies, "dom", 0, 0, tiled=True, axis_index_groups=groups)
        lines.append(line.reshape(4 * size, width))
    lines[-1], mid_rows, parent = lax.optimization_barrier((lines[-1], mid_rows, parent))
    pieces = []
    for line in lines:
        low, high = line[: 2 * size], line[2 * size :]
        low_y = cross(low)
        high_x = swap(high, 2)
        high_y = cross(high)
        low_x = swap(low, 2)
        pieces += [line, low_y, high_y, low_x, high_x, swap(low_y, 2), cross(high_x)]
    pieces = pieces + [swap(x, 1) for x in pieces]
    row = jnp.arange(CHUNKS, dtype=jnp.int32)[None, :] * size
    rel = jnp.arange(4, dtype=jnp.int32)[:, None] ^ me
    starts = spot_of(rel, 0, here >> 1, row).reshape(-1)
    return unpool(pieces, mid_rows, parent, starts, size)


def unpool(pieces, mid_rows, parent, starts, size):
    count, _ = mid_rows.shape
    total = sum(x.shape[0] for x in pieces)

    def kernel(parent_late, starts_late, mid_ref, *refs):
        refs, (out_ref, coarse_ref, wide, picked, stage, stage_c, sems) = refs[:-7], refs[-7:]
        start = 0
        for ref in refs:

            def widen(at, ref=ref, start=start):
                wide[pl.ds(start + at, 256), :] = ref[pl.ds(at, 256), :].astype(F32)

            blocks(ref.shape[0], 256, widen)
            start += ref.shape[0]
        starts_late.wait()
        for k in range(COARSE // size):
            rows = wide[pl.ds(pl.multiple_of(starts_late.ref[k], size), size), :]
            stage_c[k * size : (k + 1) * size, :] = rows.astype(BF)
        copies = [pltpu.make_async_copy(stage_c, coarse_ref, sems.at[parent_late.pieces])]
        copies[0].start()

        def gather(j):
            picked[pl.ds(j, 1), :] = wide[pl.ds(parent_late.ref[j], 1), :]

        def flush(k, rows):
            def narrow(at):
                spot = pl.ds(k * rows + at, 256)
                stage[spot, :] = (picked[spot, :] + mid_ref[spot, :].astype(F32)).astype(BF)

            blocks(rows, 256, narrow)
            spot = pl.ds(k * rows, rows)
            copies.append(pltpu.make_async_copy(stage.at[spot], out_ref.at[spot], sems.at[k]))
            copies[-1].start()

        parent_late.loop(gather, UNROLL, flush)
        for copy in copies:
            copy.wait()

    return call(
        kernel,
        (shaped(count, BF), shaped(COARSE, BF)),
        [INDEX, INDEX, VMEM] + [VMEM] * len(pieces),
        [
            shaped(total, F32),
            shaped(count, F32),
            shaped(count, BF),
            shaped(COARSE, BF),
            pltpu.SemaphoreType.DMA((pieces_of(parent, INDEX) + 1,)),
        ],
        (pl.BlockSpec(memory_space=pl.ANY), pl.BlockSpec(memory_space=pl.ANY)),
    )(parent, starts, mid_rows, *pieces)


def solution(mesh):
    placed = (
        P("dom", None),
        P(("dom", "edge"), None),
        P(("dom", "edge")),
        P(("dom", "edge")),
        P("dom", None, None),
        P(("dom", "edge"), None),
        P(("dom", "edge")),
        P(("dom", "edge")),
        P("dom", None, None),
        P("dom", None, None),
        P("dom", None, None),
        P("dom"),
        P(),
        P(),
        P(),
        P(),
        P(),
        P(),
    )

    return jax.shard_map(
        shards,
        mesh=mesh,
        in_specs=placed,
        out_specs=(P("dom", None), P("dom", None)),
        check_vma=False,
    )
```

```python
import jax
import jax.numpy as jnp
from jax import lax
from jax.experimental import pallas as pl
from jax.experimental.pallas import tpu as pltpu
from jax.sharding import PartitionSpec as P


BF = jnp.bfloat16
F32 = jnp.float32
VMEM = pl.BlockSpec(memory_space=pltpu.VMEM)
SMEM = pl.BlockSpec(memory_space=pltpu.SMEM)
HBM = pl.BlockSpec(memory_space=pltpu.HBM)
INDEX = "index"
WEIGHT = "weight"
LOAD = "load"
LATE = (INDEX, WEIGHT, LOAD)
FULL = 60 * 1024 * 1024
COARSE = 2048
UNROLL = 32
ACCS = 4
EARLY = 128


def nbytes(x):
    width = -(-x.shape[-1] // 128) * 128
    return x.size // x.shape[-1] * width * x.dtype.itemsize


class Late:
    def __init__(self, source, ref, sems):
        self.ref = ref
        self.pieces = sems.shape[0]
        self.size = source.shape[0] // self.pieces
        self.copies = []
        for k in range(self.pieces):
            at = pl.ds(k * self.size, self.size)
            self.copies.append(pltpu.make_async_copy(source.at[at], ref.at[at], sems.at[k]))
            self.copies[-1].start()

    def wait(self):
        for copy in self.copies:
            copy.wait()

    def loop(self, body, unroll, after=None):
        for k, copy in enumerate(self.copies):
            copy.wait()

            def step(i, carry, start=k * self.size):
                for j in range(unroll):
                    body(start + i * unroll + j)
                return carry

            lax.fori_loop(0, self.size // unroll, step, 0)
            if after is not None:
                after(k, self.size)


def pieces_of(x, spec):
    return x.shape[0] // 2048 if spec in (INDEX, LOAD) and x.shape[0] % 2048 == 0 else 1


def call(kernel, out_shape, in_specs, scratch=(), out_specs=None, full=False):
    def run(*args):
        late = [k for k, spec in enumerate(in_specs) if spec in LATE]
        homes = [(pltpu.SMEM if in_specs[k] is INDEX else pltpu.VMEM)(args[k].shape, args[k].dtype) for k in late]
        sems = [pltpu.SemaphoreType.DMA((pieces_of(args[k], in_specs[k]),)) for k in late]
        used = sum(nbytes(x) for x, spec in zip(args, in_specs) if spec is not INDEX)
        used += sum(nbytes(x) for x in jax.tree.leaves(out_shape))
        used += sum(nbytes(x) for x in scratch if hasattr(x, "size"))
        n_out = len(jax.tree.leaves(out_shape))

        def body(*refs):
            ins, outs = list(refs[: len(args)]), refs[len(args) : len(args) + n_out]
            mine = refs[len(args) + n_out : len(args) + n_out + len(scratch)]
            rest = refs[len(args) + n_out + len(scratch) :]
            for at, k in enumerate(late):
                ins[k] = Late(ins[k], rest[at], rest[len(late) + at])
            kernel(*ins, *outs, *mine)

        return pl.pallas_call(
            body,
            out_shape=out_shape,
            in_specs=[HBM if spec in LATE else spec for spec in in_specs],
            out_specs=out_specs or jax.tree.map(lambda x: VMEM, out_shape),
            scratch_shapes=[pltpu.VMEM(x.shape, x.dtype) if hasattr(x, "size") else x for x in scratch]
            + homes
            + sems,
            compiler_params=pltpu.CompilerParams(vmem_limit_bytes=FULL if full else used + 2 * 1024 * 1024),
        )(*args)

    return run


def shaped(rows, dtype, width=128):
    return jax.ShapeDtypeStruct((rows, width), dtype)


def dot(a, b):
    return jnp.dot(a, b, preferred_element_type=F32)


def silu(v):
    return v / (1.0 + jnp.exp(-v))


def norm(values, gain):
    center = values - jnp.mean(values, axis=-1, keepdims=True)
    spread = jnp.mean(center * center, axis=-1, keepdims=True)
    return center * lax.rsqrt(spread + 1e-05) * gain


def chunk(total, size):
    return max(k for k in range(16, min(size, total) + 1, 16) if total % k == 0)


def blocks(total, size, body):
    size = min(size, total)

    def step(i, carry):
        body(pl.multiple_of(i * size, size))
        return carry

    lax.fori_loop(0, total // size, step, 0)


def edge_gather(nodes, senders, receivers, table, w_in, level, ghost_rows):
    rows, width = nodes.shape
    count = senders.shape[0]
    mapped = table is not None
    n = 128

    def kernel(send_idx, recv_idx, w_late, nodes_late, *refs):
        if mapped:
            table_late, lines_late, refs = refs[0], refs[1], refs[2:]
            out_ref, place_ref, send_tab, recv_tab, stage, places, sems = refs
        else:
            out_ref, send_tab, recv_tab, stage, sems = refs
        send_tab[pl.ds(rows, ghost_rows), :] = jnp.zeros((ghost_rows, width), F32)
        w_late.wait()
        w_s = w_late.ref[level, 0:width, :]
        w_r = w_late.ref[level, width : 2 * width, :]
        for k, copy in enumerate(nodes_late.copies):
            copy.wait()

            def project(at, start=k * nodes_late.size):
                block = nodes_late.ref[pl.ds(start + at, 512), :]
                send_tab[pl.ds(start + at, 512), :] = dot(block, w_s)
                recv_tab[pl.ds(start + at, 512), :] = dot(block, w_r)

            blocks(nodes_late.size, 512, project)
        if mapped:
            table_late.wait()
            lines_late.wait()
            high, low = digits(table_late.ref[...])
        send_idx.wait()
        copies = []
        for k, copy in enumerate(recv_idx.copies):
            copy.wait()
            start = k * recv_idx.size

            def gather(i, carry, start=start):
                base = start + i * n
                for j in range(n):
                    s = send_idx.ref[base + j]
                    r = recv_idx.ref[base + j]
                    stage[pl.ds(base + j, 1), :] = send_tab[pl.ds(s, 1), :] + recv_tab[pl.ds(r, 1), :]
                if mapped:
                    line = pl.ds(start // n + i, 1)
                    places[line, :] = look_up(high, low, lines_late.ref[line, :])
                return carry

            lax.fori_loop(0, recv_idx.size // n, gather, 0)
            spot = pl.ds(start, recv_idx.size)
            copies.append(pltpu.make_async_copy(stage.at[spot], out_ref.at[spot], sems.at[k]))
            copies[-1].start()
        if mapped:
            copies.append(pltpu.make_async_copy(places, place_ref, sems.at[recv_idx.pieces]))
            copies[-1].start()
        for copy in copies:
            copy.wait()

    any_space = pl.BlockSpec(memory_space=pl.ANY)
    sems = pltpu.SemaphoreType.DMA((pieces_of(receivers, INDEX) + 1,))
    scratch = [shaped(rows + ghost_rows, F32), shaped(rows, F32), shaped(count, F32)]
    args = (senders, receivers, w_in, nodes)
    specs = [INDEX, INDEX, WEIGHT, LOAD]
    if not mapped:
        return call(kernel, shaped(count, F32), specs, scratch + [sems], any_space, level == 0)(*args), None
    places = shaped(count // n, jnp.int32)
    pre, place = call(
        kernel,
        (shaped(count, F32), places),
        specs + [WEIGHT, WEIGHT],
        scratch + [places, sems],
        (any_space, any_space),
        True,
    )(*args, table.reshape(-1, 128), receivers.reshape(-1, 128))
    return pre, place.reshape(-1)


def edge_message(pre, edges, ghosts, halo, senders, places, w_in, w_out, gain, level, rows, slots):
    count, width = pre.shape
    ghost_rows = ghosts.shape[0] * halo
    fourth = slots // 4
    n = 256
    total = count // n

    def kernel(recv_idx, *refs):
        (send_late, w_late, wo_late, gain_late, pre_late, edge_late, ghost_late,
         k0_ref, k2_ref, s1_ref, s3_ref, even, odd, k0_st, k2_st, s1_st, s3_st) = refs[:17]
        accs, sems = refs[17:-1], refs[-1]

        room = chunk(slots, 512)

        def clear(at):
            for acc in accs:
                acc[pl.ds(at, room), :] = jnp.zeros((room, width), F32)

        blocks(slots, room, clear)
        send_late.wait()
        w_late.wait()
        wo_late.wait()
        gain_late.wait()
        pre_late.wait()
        edge_late.wait()
        ghost_late.wait()
        w_s = w_late.ref[level, 0:width, :]
        w_e = w_late.ref[level, 2 * width : 3 * width, :]
        w_o = wo_late.ref[level]
        scale = gain_late.ref[level : level + 1, :]

        def message(b, msg):
            at = pl.multiple_of(b * n, n)
            columns = []
            for k in range(n // 128):
                far = (send_late.ref[pl.ds(b * (n // 128) + k, 1), :] - rows).astype(F32)
                columns.append(jnp.broadcast_to(far, (8, 128)).T[:, 0:1])
            column = jnp.concatenate(columns, axis=0)
            lane = lax.broadcasted_iota(jnp.int32, (n, ghost_rows), 1).astype(F32)
            pick = (column == lane).astype(BF)
            border = ghost_late.ref[:, 0:halo, :].reshape(ghost_rows, width)
            picked = dot(pick, border).astype(BF)
            first = pre_late.ref[pl.ds(at, n), :] + (dot(picked, w_s) + dot(edge_late.ref[pl.ds(at, n), :], w_e))
            msg[...] = norm(dot(silu(first).astype(BF), w_o), scale)

        def scatter(b, msg):
            base = b * n
            for j in range(n):
                acc = accs[j % ACCS]
                r = recv_idx.ref[base + j]
                acc[pl.ds(r, 1), :] = acc[pl.ds(r, 1), :] + msg[pl.ds(j, 1), :]

        message(0, even)
        recv_idx.wait()

        def step(i, carry):
            b = 2 * i
            message(b + 1, odd)
            scatter(b, even)
            message(jnp.minimum(b + 2, total - 1), even)
            scatter(b + 1, odd)
            return carry

        lax.fori_loop(0, total // 2, step, 0)
        copies = []
        outs = ((3, s3_st, s3_ref), (1, k2_st, k2_ref), (2, s1_st, s1_ref), (0, k0_st, k0_ref))
        for k, (place, stage, out_ref) in enumerate(outs):
            m = chunk(fourth, 400)

            def body(at, stage=stage, start=place * fourth, m=m):
                value = accs[0][pl.ds(at + start, m), :]
                for acc in accs[1:]:
                    value = value + acc[pl.ds(at + start, m), :]
                stage[pl.ds(at, m), :] = value.astype(stage.dtype)

            blocks(fourth, m, body)
            copies.append(pltpu.make_async_copy(stage, out_ref, sems.at[k]))
            copies[-1].start()
        for copy in copies:
            copy.wait()

    outs = (shaped(fourth, F32), shaped(fourth, F32), shaped(fourth, BF), shaped(fourth, BF))
    return call(
        kernel,
        outs,
        [INDEX] + [WEIGHT] * 4 + [LOAD] * 3,
        [shaped(n, F32), shaped(n, F32), *outs]
        + [shaped(slots, F32)] * ACCS
        + [pltpu.SemaphoreType.DMA((4,))],
        (pl.BlockSpec(memory_space=pl.ANY),) * 4,
        True,
    )(places, senders.reshape(-1, 128), w_in, w_out, gain, pre, edges, ghosts)


def node_update(rows, kept, first, second, w_in, w_out, gain, level, copies=1):
    count, width = rows.shape
    n = chunk(count, 704)
    assert copies == 1 or n == count
    head = 0 if copies == 1 else EARLY
    tail = n - head

    def kernel(rows_ref, kept_ref, first_ref, second_ref, w_ref, wo_ref, gain_ref, out_ref, *head_ref):
        own = rows_ref[...]
        total = (kept_ref[...] + first_ref[...].astype(F32) + second_ref[...].astype(F32)).astype(BF)
        hidden = silu(dot(own, w_ref[level, 0:width, :]) + dot(total, w_ref[level, width : 2 * width, :])).astype(BF)
        result = norm(dot(hidden, wo_ref[level]), gain_ref[level : level + 1, :])
        value = (own.astype(F32) + result).astype(BF)
        for ref in head_ref:
            ref[...] = value[:head]
        for k in range(copies):
            out_ref[k * tail : (k + 1) * tail, :] = value[head:]

    block = pl.BlockSpec((n, width), lambda i: (i, 0))
    return pl.pallas_call(
        kernel,
        grid=(count // n,),
        out_shape=[shaped(copies * (count - head), BF)] + [shaped(head, BF)] * (head > 0),
        in_specs=[block] * 4
        + [pl.BlockSpec(x.shape, lambda i, d=x.ndim: (0,) * d) for x in (w_in, w_out, gain)],
        out_specs=[pl.BlockSpec((copies * tail, width), lambda i: (i, 0))]
        + [pl.BlockSpec((head, width), lambda i: (i, 0))] * (head > 0),
        name="node_update",
        compiler_params=pltpu.CompilerParams(vmem_limit_bytes=FULL if level == 0 else 8 * 1024 * 1024),
    )(rows, kept, first, second, w_in, w_out, gain)


def take_rows(tables, index):
    rows = sum(x.shape[0] for x in tables)
    count = index.shape[0]

    def kernel(index_late, *refs):
        refs, (out_ref, wide, picked) = refs[:-3], refs[-3:]
        start = 0
        for ref in refs:

            m = chunk(ref.shape[0], 400)

            def widen(at, ref=ref, start=start, m=m):
                wide[pl.ds(start + at, m), :] = ref[pl.ds(at, m), :].astype(F32)

            blocks(ref.shape[0], m, widen)
            start += ref.shape[0]

        def gather(j):
            picked[pl.ds(j, 1), :] = wide[pl.ds(index_late.ref[j], 1), :]

        index_late.loop(gather, UNROLL)

        def narrow(at):
            out_ref[pl.ds(at, 256), :] = picked[pl.ds(at, 256), :].astype(BF)

        blocks(count, 256, narrow)

    return call(
        kernel, shaped(count, BF), [INDEX] + [VMEM] * len(tables), [shaped(rows, F32), shaped(count, F32)]
    )(index, *tables)


def packed_rows(nodes, index, base, room):
    rows, width = nodes.shape
    n_dom, part = index.shape
    unroll = chunk(part, 32)

    def kernel(base_late, index_late, nodes_ref, out_ref, wide, picked):
        m = chunk(room + part, 512)

        def clear(at):
            picked[pl.ds(at, m), :] = jnp.zeros((m, width), F32)

        blocks(room + part, m, clear)

        def widen(at):
            wide[pl.ds(at, 256), :] = nodes_ref[pl.ds(at, 256), :].astype(F32)

        blocks(rows, 256, widen)
        base_late.wait()
        index_late.wait()

        def group(p, carry):
            start = base_late.ref[p]

            def gather(i, c):
                at = i * unroll
                for j in range(unroll):
                    picked[pl.ds(start + at + j, 1), :] = wide[pl.ds(index_late.ref[p * part + at + j], 1), :]
                return c

            return lax.fori_loop(0, part // unroll, gather, carry)

        lax.fori_loop(0, n_dom, group, 0)
        m = chunk(room, 400)

        def narrow(at, m=m):
            out_ref[pl.ds(at, m), :] = picked[pl.ds(at, m), :].astype(BF)

        blocks(room, m, narrow)

    return call(
        kernel, shaped(room, BF), [INDEX, INDEX, VMEM], [shaped(rows, F32), shaped(room + part, F32)]
    )(base, index.reshape(-1), nodes)


def expand(packed, base, part):
    room, width = packed.shape
    n_dom = base.shape[0]

    def kernel(base_late, packed_ref, out_ref, wide):
        wide[pl.ds(room, part), :] = jnp.zeros((part, width), F32)
        m = chunk(room, 400)

        def widen(at):
            wide[pl.ds(at, m), :] = packed_ref[pl.ds(at, m), :].astype(F32)

        blocks(room, m, widen)
        base_late.wait()

        def copy(p, carry):
            rows = wide[pl.ds(base_late.ref[p], part), :]
            out_ref[pl.ds(pl.multiple_of(p * part, 16), part), :] = rows.astype(BF)
            return carry

        lax.fori_loop(0, n_dom, copy, 0)

    return call(kernel, shaped(n_dom * part, BF), [INDEX, VMEM], [shaped(room + part, F32)])(base, packed)


def layout(unpool_slot, me, n_dom, span, room):
    lines = unpool_slot.shape[0] // 128

    def kernel(me_ref, slot_ref, place_ref, base_ref):
        here = me_ref[0]
        slot = slot_ref[...]
        owner = jnp.zeros_like(slot)
        for k in range(1, n_dom):
            owner = owner + (slot >= k * span).astype(jnp.int32)
        within = slot - owner * span
        quarter = within & 3
        place = jnp.zeros_like(slot)
        starts = [jnp.int32(0)] * 4
        for k in range(n_dom):
            mine = owner == k
            count = jnp.sum(mine.astype(F32)).astype(jnp.int32)
            base = jnp.int32(0)
            for e in range(4):
                place = jnp.where(mine & (quarter == e), starts[e], place)
                base = base + jnp.where(here == e, starts[e], 0)
                starts[e] = starts[e] + ((count - e + 3) >> 2)
            base_ref[k] = base
        rel = quarter ^ here
        place_ref[...] = ((rel & 1) * 2 + (rel >> 1)) * room + place + (within >> 2)

    place, base = pl.pallas_call(
        kernel,
        out_shape=(jax.ShapeDtypeStruct((lines, 128), jnp.int32), jax.ShapeDtypeStruct((n_dom,), jnp.int32)),
        in_specs=[SMEM, VMEM],
        out_specs=(VMEM, SMEM),
        name="layout",
        compiler_params=pltpu.CompilerParams(vmem_limit_bytes=8 * 1024 * 1024),
    )(me.reshape(1), unpool_slot.reshape(lines, 128))
    return place.reshape(-1), base


def digits(table):
    return (table >> 7).astype(F32).T.astype(BF), (table & 127).astype(F32).T.astype(BF)


def look_up(high, low, at):
    pick = (lax.broadcasted_iota(jnp.int32, (high.shape[1], 128), 0) == (at >> 7)).astype(BF)
    value = dot(high, pick) * 128.0 + dot(low, pick)
    lane = lax.broadcasted_iota(jnp.int32, (128, 128), 0) == (at & 127)
    return jnp.sum(jnp.where(lane, value, 0.0), axis=0, keepdims=True).astype(jnp.int32)


def resolve(table, index):
    lines = index.shape[0] // 128
    tall = table.shape[0] // 128

    def kernel(table_ref, index_ref, out_ref):
        high, low = digits(table_ref[...])

        def step(i, carry):
            for k in range(8):
                out_ref[pl.ds(i * 8 + k, 1), :] = look_up(high, low, index_ref[pl.ds(i * 8 + k, 1), :])
            return carry

        lax.fori_loop(0, lines // 8, step, 0)

    out = jax.ShapeDtypeStruct((lines, 128), jnp.int32)
    return call(kernel, out, [VMEM, VMEM], ())(table.reshape(tall, 128), index.reshape(lines, 128)).reshape(-1)


def pool_sum(arrived, places, bit):
    count, _ = arrived.shape
    n = 256
    half = COARSE // 2

    def kernel(bit_late, arrived_ref, places_late, mine_ref, theirs_ref):
        places_late.wait()
        bit_late.wait()
        rows = arrived_ref[...]
        for out_ref, start in ((theirs_ref, (1 - bit_late.ref[0]) * half), (mine_ref, bit_late.ref[0] * half)):

            def step(at, out_ref=out_ref, start=start):
                near = jnp.clip(places_late.ref[...] - (start + at), -1, n).astype(F32).astype(BF)
                row = lax.broadcasted_iota(jnp.int32, (n, count), 0).astype(F32).astype(BF)
                pick = jnp.where(near == row, jnp.ones((), BF), jnp.zeros((), BF))
                out_ref[pl.ds(at, n), :] = dot(pick, rows)

            blocks(half, n, step)

    return call(kernel, (shaped(half, F32), shaped(half, F32)), [INDEX, VMEM, WEIGHT], ())(
        bit.reshape(1), arrived, places.reshape(1, count)
    )


def child_count(places):
    high = (places // 128)[None, :] == jnp.arange(COARSE // 128, dtype=jnp.int32)[:, None]
    low = (places % 128)[:, None] == jnp.arange(128, dtype=jnp.int32)[None, :]
    return dot(high.astype(BF), low.astype(BF)).reshape(COARSE)


def swap(x, bit):
    size = lax.axis_size("edge")
    return lax.ppermute(x, "edge", [(i, i ^ bit) for i in range(size)])


def layer_sums(nodes, edges, senders, receivers, border, level, w, slots, table, extra=None):
    rows, width = nodes.shape
    n_dom, halo = border.shape[1:]
    outgoing = nodes[border[0].reshape(-1)].reshape(n_dom, halo, width)
    if extra is not None:
        outgoing = jnp.concatenate([outgoing, extra], axis=1)
    arrived = lax.all_to_all(outgoing, "dom", split_axis=0, concat_axis=0, tiled=True)
    pre, places = edge_gather(nodes, senders, receivers, table, w[0], level, n_dom * halo)
    if table is None:
        me = lax.axis_index("edge")
        quarter = rows // 4
        places = order_of((receivers // quarter) ^ me) * quarter + receivers % quarter
    k0, k2, s1, s3 = edge_message(pre, edges, arrived, halo, senders, places, w[0], w[1], w[4], level, rows, slots)
    second = swap((k2 + swap(s3, 1).astype(F32)).astype(BF), 2)
    return k0, swap(s1, 1), second, arrived


def order_of(rel):
    return (rel & 1) * 2 + (rel >> 1)


def shards(
    fine_nodes,
    fine_edges,
    fine_senders,
    fine_receivers,
    fine_halo,
    coarse_edges,
    coarse_senders,
    coarse_receivers,
    coarse_halo,
    pool_send,
    pool_dest,
    unpool_slot,
    edge_in_weight,
    edge_out_weight,
    node_in_weight,
    node_out_weight,
    edge_gain,
    node_gain,
):
    w = (edge_in_weight, edge_out_weight, node_in_weight, node_out_weight, edge_gain, node_gain)
    width = fine_nodes.shape[-1]
    n_dom = pool_send.shape[1]
    span = pool_send.shape[2]
    part = span // 4
    me = lax.axis_index("edge")
    direct = n_dom == 8 and span % 128 == 0 and fine_halo.shape[2] % 16 == 0
    room = -(-(fine_nodes.shape[0] // 4 + n_dom) // 64) * 64
    slot_place, base = layout(unpool_slot, me, n_dom, span, room)

    def own_quarter(lists):
        return lax.dynamic_index_in_dim(lists[0].reshape(n_dom, part, 4), me, 2, keepdims=False)

    my_dest = own_quarter(pool_dest).reshape(-1)
    counts = child_count(pool_dest[0].reshape(-1))
    scale = jnp.maximum(counts, 1.0)[:, None]

    extra = None
    if direct:
        lists = pool_dest[0].reshape(n_dom, span // 128, 128)
        digit = [(lists >> 7).astype(BF), (lists & 127).astype(BF)]
        extra = jnp.concatenate(digit + [jnp.zeros((n_dom, -2 * (span // 128) % 16, 128), BF)], axis=1)
    kept, first, second, arrived_lists = layer_sums(
        fine_nodes, fine_edges, fine_senders, fine_receivers, fine_halo, 0, w, 4 * room, slot_place, extra
    )
    sends, kept = lax.optimization_barrier((pool_send, kept))
    own = packed_rows(fine_nodes, own_quarter(sends), base, room)
    (mid,) = node_update(own, kept, first, second, w[2], w[3], w[5], 0)
    if direct:
        mid_x = swap(mid, 2)
    spread = expand(mid, base, part)
    arrived = lax.all_to_all(spread.reshape(n_dom, part, width), "dom", split_axis=0, concat_axis=0, tiled=True)
    if direct:
        lists, _ = lax.optimization_barrier((arrived_lists, spread))
        n = span // 128
        digit = lists[:, fine_halo.shape[2] : fine_halo.shape[2] + 2 * n].astype(jnp.int32)
        known = (digit[:, :n] * 128 + digit[:, n:]).reshape(-1, span)
        parent = resolve(place_of(known), unpool_slot)
        my_dest, parent = lax.optimization_barrier((my_dest, parent))
    bit = me & 1
    half = COARSE // 2
    mine, theirs = pool_sum(arrived.reshape(-1, width), my_dest, bit)
    mine = mine + swap(theirs, 1)
    mine = mine + swap(mine.astype(BF), 2).astype(F32)
    mine = (mine / lax.dynamic_slice_in_dim(scale, bit * half, half, 0)).astype(BF)
    if direct:
        mine, mid, mid_1, mid_3 = lax.optimization_barrier((mine, mid, swap(mid, 1), swap(mid_x, 1)))
    theirs = swap(mine, 1)
    coarse_in = jnp.concatenate([jnp.where(bit == 0, mine, theirs), jnp.where(bit == 0, theirs, mine)], axis=0)

    kept, first, second, _ = layer_sums(
        coarse_in, coarse_edges, coarse_senders, coarse_receivers, coarse_halo, 1, w, COARSE, None
    )
    fourth = COARSE // 4
    own = lax.dynamic_slice_in_dim(coarse_in, me * fourth, fourth, 0)
    top = node_update(own, kept, first, second, w[2], w[3], w[5], 1, 4 if direct else 1)
    if direct:
        return spread_out(top, [mid, mid_x, mid_1, mid_3], slot_place, parent)

    coarse_out = lax.all_gather(top[0], "edge", axis=0, tiled=True)
    parents = take_rows([coarse_out], jnp.minimum(my_dest, COARSE - 1))
    back = lax.all_to_all(parents.reshape(n_dom, part, width), "dom", split_axis=0, concat_axis=0, tiled=True)
    final = (spread.astype(F32) + back.reshape(-1, width).astype(F32)).astype(BF)
    final_x = swap(final, 2)
    within = unpool_slot % span
    place = order_of((within % 4) ^ me) * (n_dom * part) + (unpool_slot // span) * part + within // 4
    fine_out = take_rows([final, final_x, swap(final, 1), swap(final_x, 1)], place)
    return (fine_out, coarse_out)


def late_spot(rel, dy, z, row):
    size = COARSE // 4 - EARLY
    return (rel & 1) * (4 * COARSE) + ((rel >> 1) * 2 + dy) * (4 * size) + z * size + row - EARLY


def early_spot(rel, dy, z, row):
    here = lax.axis_index("dom") >> 1
    size = COARSE // 4 - EARLY
    return (rel & 1) * (4 * COARSE) + 16 * size + ((here - z) & 3) * (4 * EARLY) + ((rel >> 1) * 2 + dy) * EARLY + row


def place_of(known):
    me = lax.axis_index("edge")
    here = lax.axis_index("dom")
    fourth = COARSE // 4
    owner = jnp.arange(known.shape[0], dtype=jnp.int32)[:, None]
    at = ((known // fourth) ^ me, (owner ^ here) & 1, owner >> 1, known % fourth)
    return jnp.where(at[3] < EARLY, early_spot(*at), late_spot(*at)).reshape(-1)


def spread_out(top, mids, slot_place, parent):
    late, early = top
    width = early.shape[1]
    size = late.shape[0] // 4
    me = lax.axis_index("edge")
    here = lax.axis_index("dom")
    groups = [[0, 2, 4, 6], [1, 3, 5, 7]]

    def cross(x):
        return lax.ppermute(x, "dom", [(i, i ^ 1) for i in range(8)])

    def over_x(x):
        return swap(x, 2)

    early_y = cross(early)
    early_x = over_x(early)
    line = lax.all_to_all(
        late.reshape(4, size, width), "dom", 0, 0, tiled=True, axis_index_groups=groups
    ).reshape(4 * size, width)
    square = jnp.concatenate([early, early_y, early_x, over_x(early_y)], axis=0)
    slot_place, _ = lax.optimization_barrier((slot_place, late))
    mid_rows = take_rows(mids, slot_place)
    line, square, mid_rows = lax.optimization_barrier((line, square, mid_rows))
    low, high = line[: 2 * size], line[2 * size :]
    low_y, high_x = cross(low), over_x(high)
    squares = [square]
    for k in range(1, 4):
        squares.append(lax.ppermute(square, "dom", [(i, (i + 2 * k) % 8) for i in range(8)]))
    high_y, low_x = cross(high), over_x(low)
    corner_x, corner_y = over_x(low_y), cross(high_x)
    partner_x = swap(corner_x, 1)
    partner_y = swap(corner_y, 1)
    first = [line, low_y, high_y, low_x, high_x]
    pieces = first + [corner_x, corner_y] + squares
    pieces += [swap(x, 1) for x in first] + [partner_x, partner_y, swap(square, 1)]
    for x in squares[1:]:
        pieces.append(swap(x, 1))
    rel = jnp.arange(4, dtype=jnp.int32) ^ me
    starts = jnp.concatenate([early_spot(rel, 0, here >> 1, 0), late_spot(rel, 0, here >> 1, EARLY)])
    return unpool(pieces, mid_rows, parent, starts)


def unpool(pieces, mid_rows, parent, starts):
    count, _ = mid_rows.shape
    total = sum(x.shape[0] for x in pieces)

    def kernel(parent_late, starts_late, *refs):
        mid_late, refs = refs[-8], refs[:-8] + refs[-7:]
        refs, (out_ref, coarse_ref, wide, picked, stage, stage_c, sems) = refs[:-7], refs[-7:]
        start = 0
        for ref in refs:

            ref.wait()

            def widen(at, ref=ref.ref, start=start):
                wide[pl.ds(start + at, 256), :] = ref[pl.ds(at, 256), :].astype(F32)

            blocks(ref.ref.shape[0], 256, widen)
            start += ref.ref.shape[0]
        starts_late.wait()
        fourth = COARSE // 4
        for k in range(8):
            first, rows = ((k & 3) * fourth, EARLY) if k < 4 else ((k & 3) * fourth + EARLY, fourth - EARLY)
            found = wide[pl.ds(pl.multiple_of(starts_late.ref[k], 128), rows), :]
            stage_c[first : first + rows, :] = found.astype(BF)
        copies = [pltpu.make_async_copy(stage_c, coarse_ref, sems.at[parent_late.pieces])]
        copies[0].start()

        def gather(j):
            picked[pl.ds(j, 1), :] = wide[pl.ds(parent_late.ref[j], 1), :]

        assert mid_late.pieces == parent_late.pieces

        def flush(k, rows):
            mid_late.copies[k].wait()

            def narrow(at):
                spot = pl.ds(k * rows + at, 256)
                stage[spot, :] = (picked[spot, :] + mid_late.ref[spot, :].astype(F32)).astype(BF)

            blocks(rows, 256, narrow)
            spot = pl.ds(k * rows, rows)
            copies.append(pltpu.make_async_copy(stage.at[spot], out_ref.at[spot], sems.at[k]))
            copies[-1].start()

        parent_late.loop(gather, UNROLL, flush)
        for copy in copies:
            copy.wait()

    return call(
        kernel,
        (shaped(count, BF), shaped(COARSE, BF)),
        [INDEX, INDEX] + [LOAD] * len(pieces) + [LOAD],
        [
            shaped(total, F32),
            shaped(count, F32),
            shaped(count, BF),
            shaped(COARSE, BF),
            pltpu.SemaphoreType.DMA((pieces_of(parent, INDEX) + 1,)),
        ],
        (pl.BlockSpec(memory_space=pl.ANY), pl.BlockSpec(memory_space=pl.ANY)),
        True,
    )(parent, starts, *pieces, mid_rows)


def solution(mesh):
    placed = (
        P("dom", None),
        P(("dom", "edge"), None),
        P(("dom", "edge")),
        P(("dom", "edge")),
        P("dom", None, None),
        P(("dom", "edge"), None),
        P(("dom", "edge")),
        P(("dom", "edge")),
        P("dom", None, None),
        P("dom", None, None),
        P("dom", None, None),
        P("dom"),
        P(),
        P(),
        P(),
        P(),
        P(),
        P(),
    )

    return jax.shard_map(
        shards,
        mesh=mesh,
        in_specs=placed,
        out_specs=(P("dom", None), P("dom", None)),
        check_vma=False,
    )
```
